256 devices in a mesh: gy: 16 (over y_lo, x, core), gx: 16 (over y_hi, z).
Axes of the slice: x: 4, y: 4 (y_hi: 2, y_lo: 2; y = y_hi * 2 + y_lo), z: 8, core: 2. Of those that a mesh axis runs over, the one named last changes fastest.
Arguments:
- tracer: float32 [8, 2048, 4096], P(None, 'gy', 'gx'), may hold values from -6 to 6
- east_speed: float32 [8, 2048, 4096], P(None, 'gy', 'gx'), may hold values from -0.25 to 0.25
- north_speed: float32 [8, 2048, 4096], P(None, 'gy', 'gx'), may hold values from -0.25 to 0.25
- columns: int32 [2048, 4096], P('gy', 'gx'), may hold values from 0 to 8
- thickness: float32 [8], replicated, may hold values from 0.5 to 2
- surface_flux: float32 [2048, 4096], P('gy', 'gx'), may hold values from -6 to 6
- helm: float32 [2048, 4096], P('gy', 'gx'), may hold values from 0.2 to 4
Outputs:
- tracer_new: float32 [8, 2048, 4096], P(None, 'gy', 'gx')
- heights: float32 [2048, 4096], P('gy', 'gx')
The draws below stay inside these ranges and needn't reach their ends.
Inputs may be any that keep to these rules, and one draw needn't show every extreme that they name: `columns`: ocean levels per column; 0 means land.
All inputs are finite; a program needn't handle non-finite values.
Results may differ from the reference program's by a relative error of at most 0.0001.
Values sent between devices are 32-bit elements; how exact they have to be, the bound alone decides.
A program may use at most 64 MiB of HBM per device.

```python
import math
import jax
import jax.numpy as jnp
from jax import lax

K = 8
TSTEPS = 2
ITERS = 3
NY = 2048
NX = 4096


def plant(entries, own_key, smallest, top_value):
    shape = entries.shape
    index_at = [jax.random.randint(jax.random.fold_in(own_key, axis), (), 0, shape[axis]) for axis in range(len(shape))]
    entries = entries.at[tuple(index_at)].set(smallest)
    longest = shape.index(max(shape))
    index_at[longest] = (index_at[longest] + 1) % shape[longest]
    return entries.at[tuple(index_at)].set(top_value)


def block_levels(stream_key, shape, split, least, top_value):
    def one(dim, blocks):
        steps = jax.random.uniform(jax.random.fold_in(jax.random.fold_in(stream_key, 6), dim), (blocks,), jnp.float32, least / len(split), top_value / len(split))
        return jnp.repeat(jnp.exp(steps), shape[dim] // blocks).reshape((-1,) + (1,) * (len(shape) - dim - 1))

    loudness = one(*split[0])
    for cut in split[1:]:
        loudness = loudness * one(*cut)
    return loudness


def normal_values(own_key, extent, width, bound, pieces=(), kind=jnp.bfloat16):
    drawn = width * jax.random.normal(own_key, extent, jnp.float32)
    if pieces:
        drawn = drawn * block_levels(own_key, extent, pieces, -0.22, 0.18)
    return jnp.clip(drawn, -bound, bound).astype(kind)


def setup_inputs(seed: int = 0) -> dict:
    arg_keys = jax.random.split(jax.random.key(seed), 8)
    return {
        "tracer": normal_values(arg_keys[0], (K, NY, NX), 1.0, 6.0, ((1, 16), (2, 16)), jnp.float32),
        "east_speed": jnp.clip(jax.random.uniform(arg_keys[1], (K, NY, NX), jnp.float32, -0.25, 0.25) * block_levels(arg_keys[1], (K, NY, NX), ((1, 16), (2, 16)), -0.4, 0.0), -0.25, 0.25),
        "north_speed": jnp.clip(jax.random.uniform(arg_keys[2], (K, NY, NX), jnp.float32, -0.25, 0.25) * block_levels(arg_keys[2], (K, NY, NX), ((1, 16), (2, 16)), -0.4, 0.0), -0.25, 0.25),
        "columns": plant(jax.random.randint(arg_keys[3], (NY, NX), 0, K + 1), jax.random.fold_in(arg_keys[3], 1), 0, K).astype(jnp.int32),
        "thickness": jnp.clip(jnp.exp(jax.random.uniform(arg_keys[4], (K,), jnp.float32, math.log(0.5), math.log(2.0))), 0.5, 2.0),
        "surface_flux": normal_values(arg_keys[5], (NY, NX), 1.0, 6.0, ((0, 16), (1, 16)), jnp.float32),
        "helm": jnp.clip(jnp.exp(math.log(4.0) - 2.9957323 * jax.random.uniform(arg_keys[6], (NY, NX), jnp.float32) ** block_levels(arg_keys[6], (NY, NX), ((0, 16), (1, 16)), -0.2, 0.2)), 0.2, 4.0),
    }


def upwind(speed, behind, ahead):
    return jnp.maximum(speed, 0.0) * behind + jnp.minimum(speed, 0.0) * ahead


def advect(current, east_speed, north_speed, ocean):
    tracer_east = jnp.roll(current, -1, axis=2)
    ocean_east = jnp.roll(ocean, -1, axis=2)
    tracer_north = jnp.pad(current[:, 1:, :], ((0, 0), (0, 1), (0, 0)))
    ocean_north = jnp.pad(ocean[:, 1:, :], ((0, 0), (0, 1), (0, 0)))
    flux_east = ocean * ocean_east * upwind(east_speed, current, tracer_east)
    flux_north = ocean * ocean_north * upwind(north_speed, current, tracer_north)
    flux_west = jnp.roll(flux_east, 1, axis=2)
    flux_south = jnp.pad(flux_north[:, :-1, :], ((0, 0), (1, 0), (0, 0)))
    return current - (flux_east - flux_west + flux_north - flux_south)


def neighbour(source, row_step, col_step):
    moved = jnp.roll(source, -col_step, axis=1)
    if row_step == 1:
        moved = jnp.pad(moved[1:], ((0, 1), (0, 0)))
    elif row_step == -1:
        moved = jnp.pad(moved[:-1], ((1, 0), (0, 0)))
    return moved


def nine_point(source, wet, diagonal_term):
    weighted = wet * source
    edges = neighbour(weighted, 0, 1) + neighbour(weighted, 0, -1) + neighbour(weighted, 1, 0) + neighbour(weighted, -1, 0)
    corners = neighbour(weighted, 1, 1) + neighbour(weighted, 1, -1) + neighbour(weighted, -1, 1) + neighbour(weighted, -1, -1)
    return diagonal_term * source - wet * (edges + 0.5 * corners)


def reference(tracer, east_speed, north_speed, columns, thickness, surface_flux, helm):
    depth = lax.broadcasted_iota(jnp.int32, tracer.shape, 0)
    ocean = (depth < columns[None]).astype(jnp.float32)
    current = tracer
    for section_index in range(TSTEPS):
        current = advect(current, east_speed, north_speed, ocean)
    forcing = surface_flux + jnp.sum(thickness[:, None, None] * ocean * current, axis=0)
    wet = ocean[0]
    diagonal_term = 6.0 + helm
    heights = jnp.zeros_like(forcing)
    residual = forcing
    scaled = residual / diagonal_term
    direction = scaled
    product_now = jnp.sum(residual * scaled)
    for iteration in range(ITERS):
        applied = nine_point(direction, wet, diagonal_term)
        step_size = product_now / jnp.sum(direction * applied)
        heights = heights + step_size * direction
        residual = residual - step_size * applied
        scaled = residual / diagonal_term
        product_next = jnp.sum(residual * scaled)
        direction = scaled + (product_next / product_now) * direction
        product_now = product_next
    return current, heights
```

```python
import functools

import jax
import jax.numpy as jnp
from jax import lax
from jax.experimental import pallas as pl
from jax.experimental.pallas import tpu as pltpu
from jax.sharding import PartitionSpec as P

TSTEPS = 2
ITERS = 3
K = 8
R, C = 128, 256
RE, CE = R + 16, C + 128
HALO = 5
MESH = pl.DeviceIdType.MESH
TR, EA, NO, SF, HE, CO = 0, K, 2 * K, 3 * K, 3 * K + 1, 3 * K + 2
NF = 3 * K + 2


def lane_plan():
    first, last = [], []
    for plan, widths in ((first, (5, 4, 4)), (last, (5, 5, 4))):
        lane = 0
        for base, width in zip((TR, EA, NO), widths):
            for k in range(K):
                plan.append((base + k, width, lane))
                lane += width
        for field, width in ((SF, 3), (HE, 3), (CO, 5)):
            plan.append((field, width, lane))
            lane += width
        assert lane <= 128
    return first, last


FIRST, LAST = lane_plan()


def up(now, nxt, sub):
    return pltpu.roll(jnp.where(sub == 0, nxt, now), 7, 0)


def down(now, prv, sub):
    return pltpu.roll(jnp.where(sub == 7, prv, now), 1, 0)


def east(a):
    return pltpu.roll(a, CE - 1, 1)


def west(a):
    return pltpu.roll(a, 1, 1)


def kernel(
    ngy, ngx,
    tr_hbm, ea_hbm, no_hbm, co_hbm, th, sf_hbm, he_hbm,
    tr_out, h_out,
    a, ci, c1, pw, pe, re, rw, me_s, mn_s, f_s, inv_s, v1_s, v2_s, row, b1, b2,
    load_sem, send_sem, recv_sem, rs_sem, rr_sem,
):
    gy, gx = lax.axis_index("gy"), lax.axis_index("gx")
    north, south = lax.rem(gy + 1, ngy), lax.rem(gy + ngy - 1, ngy)
    e_id, w_id = lax.rem(gx + 1, ngx), lax.rem(gx + ngx - 1, ngx)
    hi, z = lax.div(gx, 8), lax.rem(gx, 8)
    group1 = [
        (lax.rem(gy + dy, ngy), lax.rem(gx + 8 * dh, ngx))
        for dh in range(2) for dy in range(16) if dy or dh
    ]
    group2 = [(gy, hi * 8 + lax.rem(z + dz, 8)) for dz in range(1, 8)]
    near = [(north, gx), (south, gx), (gy, e_id), (gy, w_id),
            (north, e_id), (north, w_id), (south, e_id), (south, w_id)]

    barrier = pltpu.get_barrier_semaphore()
    for y, x in near + group1 + group2:
        pl.semaphore_signal(barrier, inc=1, device_id={"gy": y, "gx": x}, device_id_type=MESH)

    own = (pl.ds(8, R), pl.ds(0, C))
    loads = [
        pltpu.make_async_copy(src, dst, load_sem.at[i])
        for i, (src, dst) in enumerate((
            (tr_hbm, a.at[(pl.ds(TR, K),) + own]),
            (ea_hbm, a.at[(pl.ds(EA, K),) + own]),
            (no_hbm, a.at[(pl.ds(NO, K),) + own]),
            (sf_hbm, a.at[(SF,) + own]),
            (he_hbm, a.at[(HE,) + own]),
            (co_hbm, ci.at[own]),
        ))
    ]
    for copy in loads:
        copy.start()
    for copy in loads:
        copy.wait()

    lane = lax.broadcasted_iota(jnp.int32, (R, 128), 1)

    def edge(field, side):
        cols = pl.ds(0 if side == 0 else C - 128, 128)
        if field == CO:
            return ci[pl.ds(8, R), cols].astype(jnp.float32)
        return a[field, pl.ds(8, R), cols]

    for side, plan, dest in ((0, FIRST, pw), (1, LAST, pe)):
        tile = jnp.zeros((R, 128), jnp.float32)
        for field, width, at in plan:
            start = 0 if side == 0 else 128 - width
            value = edge(field, side)
            shift = (at - start) % 128
            if shift:
                value = pltpu.roll(value, shift, 1)
            tile = jnp.where((lane >= at) & (lane < at + width), value, tile)
        dest[...] = tile

    pl.semaphore_wait(barrier, len(near) + len(group1) + len(group2))

    top, bottom = pl.ds(R, 8), pl.ds(8, 8)
    ghost_s, ghost_n = pl.ds(0, 8), pl.ds(R + 8, 8)
    cols = pl.ds(0, C)
    every = pl.ds(0, NF)
    routes = [
        (pe, rw.at[pl.ds(8, R)], (gy, e_id)),
        (pw, re.at[pl.ds(8, R)], (gy, w_id)),
        (a.at[every, top, cols], a.at[every, ghost_s, cols], (north, gx)),
        (a.at[every, bottom, cols], a.at[every, ghost_n, cols], (south, gx)),
        (ci.at[top, cols], ci.at[ghost_s, cols], (north, gx)),
        (ci.at[bottom, cols], ci.at[ghost_n, cols], (south, gx)),
        (pe.at[pl.ds(R - 8, 8)], rw.at[ghost_s], (north, e_id)),
        (pw.at[pl.ds(R - 8, 8)], re.at[ghost_s], (north, w_id)),
        (pe.at[pl.ds(0, 8)], rw.at[ghost_n], (south, e_id)),
        (pw.at[pl.ds(0, 8)], re.at[ghost_n], (south, w_id)),
    ]
    sends = [
        pltpu.make_async_remote_copy(
            src_ref=src, dst_ref=dst, send_sem=send_sem.at[i], recv_sem=recv_sem.at[i],
            device_id={"gy": y, "gx": x}, device_id_type=MESH,
        )
        for i, (src, dst, (y, x)) in enumerate(routes)
    ]
    for copy in sends:
        copy.start()
    for copy in sends:
        copy.wait_recv()

    lane_e = lax.broadcasted_iota(jnp.int32, (RE, 128), 1)
    last_at = {field: (width, at) for field, width, at in LAST}
    ghost = pl.ds(C, 128)
    for field, width, at in FIRST:
        from_east = re[...]
        if at:
            from_east = pltpu.roll(from_east, 128 - at, 1)
        wide, at_w = last_at[field]
        shift = (128 - wide - at_w) % 128
        from_west = rw[...]
        if shift:
            from_west = pltpu.roll(from_west, shift, 1)
        value = jnp.where(lane_e < 64, from_east, from_west)
        a[field, :, ghost] = value
    a[CO, :, cols] = ci[:, cols].astype(jnp.float32)
    zero8 = jnp.zeros((8, CE), jnp.float32)

    @pl.when(gy == 0)
    def _():
        a[CO, ghost_s, :] = zero8

    @pl.when(gy == ngy - 1)
    def _():
        a[CO, ghost_n, :] = zero8

    sub = lax.broadcasted_iota(jnp.int32, (8, CE), 0)
    tiles = RE // 8

    def rows(t):
        return pl.ds(8 * t, 8)

    for t in range(tiles):
        depth = a[CO, rows(t), :]
        above = a[CO, rows(min(t + 1, tiles - 1)), :]
        me_s[rows(t), :] = jnp.minimum(depth, east(depth))
        mn_s[rows(t), :] = jnp.minimum(depth, up(depth, above, sub))
        f_s[rows(t), :] = a[SF, rows(t), :]
        inv_s[rows(t), :] = 1.0 / (6.0 + a[HE, rows(t), :])

    def level(k, carry):
        kf = k.astype(jnp.float32)
        weight = th[k]

        def step(load, store):
            now = load(0)
            south_flux = jnp.zeros((8, CE), jnp.float32)
            for t in range(tiles):
                nxt = load(t + 1) if t + 1 < tiles else now
                es = jnp.where(me_s[rows(t), :] > kf, a[EA + k, rows(t), :], 0.0)
                ns = jnp.where(mn_s[rows(t), :] > kf, a[NO + k, rows(t), :], 0.0)
                fe = es * jnp.where(es > 0.0, now, east(now))
                fn = ns * jnp.where(ns > 0.0, now, up(now, nxt, sub))
                store(t, now - (fe - west(fe) + fn - down(fn, south_flux, sub)))
                now, south_flux = nxt, fn

        def put1(t, value):
            c1[rows(t), :] = value

        def put2(t, value):
            if 0 < t < tiles - 1:
                tr_out[k, pl.ds(8 * t - 8, 8), :] = value[:, :C]
            f_s[rows(t), :] += jnp.where(a[CO, rows(t), :] > kf, weight * value, 0.0)

        step(lambda t: a[TR + k, rows(t), :], put1)
        step(lambda t: c1[rows(t), :], put2)
        return carry

    lax.fori_loop(0, K, level, 0)

    nu = [jnp.zeros((8, C), jnp.float32) for _ in range(6)]
    for t in range(tiles):
        forcing = f_s[rows(t), :]
        z0 = forcing * inv_s[rows(t), :]
        if 0 < t < tiles - 1:
            nu[0] += (forcing * z0)[:, :C]
        c1[rows(t), :] = z0
        mn_s[rows(t), :] = jnp.where(a[CO, rows(t), :] > 0.0, 1.0, 0.0)

    def operator(src, store):
        def part(t):
            wet = mn_s[rows(t), :]
            w = wet * src[rows(t), :]
            h = west(w) + east(w)
            return wet, h, w + 0.5 * h

        wet, h, s = part(0)
        before = jnp.zeros_like(s)
        for t in range(tiles):
            after = part(t + 1) if t + 1 < tiles else (wet, h, s)
            store(t, wet * (h + up(s, after[2], sub) + down(s, before, sub)))
            before = s
            wet, h, s = after

    def store1(t, u):
        v = u * inv_s[rows(t), :]
        v1_s[rows(t), :] = v
        if 0 < t < tiles - 1:
            nu[1] += (v * f_s[rows(t), :])[:, :C]
            nu[2] += (v * u)[:, :C]

    def store2(t, u):
        v = u * inv_s[rows(t), :]
        v2_s[rows(t), :] = v
        if 0 < t < tiles - 1:
            nu[3] += (v1_s[rows(t), :] * u)[:, :C]
            nu[4] += (v * u)[:, :C]

    def store3(t, u):
        if 0 < t < tiles - 1:
            nu[5] += (v2_s[rows(t), :] * u)[:, :C]

    operator(c1, store1)
    operator(v1_s, store2)
    operator(v2_s, store3)

    lane1 = lax.broadcasted_iota(jnp.int32, (1, 128), 1)
    packed = jnp.zeros((1, 128), jnp.float32)
    for i, part in enumerate(nu):
        lanes = jnp.sum(part[:, :128] + part[:, 128:], axis=0, keepdims=True)
        total = jnp.sum(lanes, axis=1, keepdims=True)
        packed = jnp.where(lane1 == i, total, packed)

    reduce_sends = []
    for i, (group, slot, buf) in enumerate(((group1, gy * 2 + hi, b1), (group2, z, b2))):
        row[i] = packed
        n = len(group)
        for y, x in group:
            copy = pltpu.make_async_remote_copy(
                src_ref=row.at[i], dst_ref=buf.at[slot], send_sem=rs_sem.at[i], recv_sem=rr_sem.at[i],
                device_id={"gy": y, "gx": x}, device_id_type=MESH,
            )
            copy.start()
        buf[slot] = packed
        pltpu.make_async_copy(buf.at[pl.ds(0, n)], buf.at[pl.ds(0, n)], rr_sem.at[i]).wait()
        reduce_sends.append((buf, n, i))
        packed = jnp.sum(buf[...], axis=0)

    m = [jnp.sum(jnp.where(lane1 == i, packed, 0.0), axis=1, keepdims=True) for i in range(6)]

    def form(p, moments):
        total = None
        for i, pi in enumerate(p):
            for j, pj in enumerate(p[i:], i):
                term = (pi * pj if i == j else 2.0 * pi * pj) * moments[i + j]
                total = term if total is None else total + term
        return total

    diff = [m[i] - m[i + 1] for i in range(5)]
    one = jnp.ones_like(m[0])
    zc, pc = [one], [one]
    heights = [jnp.zeros_like(one)] * 3
    rz = m[0]
    for it in range(ITERS):
        alpha = rz / form(pc, diff)
        heights = [h + alpha * pc[i] if i < len(pc) else h for i, h in enumerate(heights)]
        if it + 1 < ITERS:
            applied = [p - q for p, q in zip(pc + [jnp.zeros_like(one)], [jnp.zeros_like(one)] + pc)]
            zc = [(zc[i] if i < len(zc) else 0.0) - alpha * applied[i] for i in range(len(applied))]
            rz_next = form(zc, m)
            beta = rz_next / rz
            pc = [zc[i] + beta * pc[i] if i < len(pc) else zc[i] for i in range(len(zc))]
            rz = rz_next

    inner = pl.ds(8, R)
    h_out[...] = heights[0] * c1[inner, cols] + heights[1] * v1_s[inner, cols] + heights[2] * v2_s[inner, cols]

    for copy in sends:
        copy.wait_send()
    for buf, n, i in reduce_sends:
        pltpu.make_async_copy(buf.at[pl.ds(0, n)], buf.at[pl.ds(0, n)], rs_sem.at[i]).wait()


def on_device(ngy, ngx, tracer, east_speed, north_speed, columns, thickness, surface_flux, helm):
    f32 = jnp.float32
    any_spec = pl.BlockSpec(memory_space=pltpu.HBM)
    vmem = pl.BlockSpec(memory_space=pltpu.VMEM)
    return pl.pallas_call(
        functools.partial(kernel, ngy, ngx),
        out_shape=(jax.ShapeDtypeStruct((K, R, C), f32), jax.ShapeDtypeStruct((R, C), f32)),
        in_specs=[any_spec, any_spec, any_spec, any_spec, pl.BlockSpec(memory_space=pltpu.SMEM), any_spec, any_spec],
        out_specs=(vmem, vmem),
        scratch_shapes=[
            pltpu.VMEM((NF + 1, RE, CE), f32),
            pltpu.VMEM((RE, C), jnp.int32),
            pltpu.VMEM((RE, CE), f32),
            pltpu.VMEM((R, 128), f32),
            pltpu.VMEM((R, 128), f32),
            pltpu.VMEM((RE, 128), f32),
            pltpu.VMEM((RE, 128), f32),
        ] + [pltpu.VMEM((RE, CE), f32)] * 6 + [
            pltpu.VMEM((2, 1, 128), f32),
            pltpu.VMEM((32, 1, 128), f32),
            pltpu.VMEM((8, 1, 128), f32),
            pltpu.SemaphoreType.DMA((6,)),
            pltpu.SemaphoreType.DMA((10,)),
            pltpu.SemaphoreType.DMA((10,)),
            pltpu.SemaphoreType.DMA((2,)),
            pltpu.SemaphoreType.DMA((2,)),
        ],
        compiler_params=pltpu.CompilerParams(collective_id=0, has_side_effects=True),
    )(tracer, east_speed, north_speed, columns, thickness, surface_flux, helm)


def solution(mesh):
    sizes = mesh.shape
    cells, plane = P(None, "gy", "gx"), P("gy", "gx")
    return jax.shard_map(
        functools.partial(on_device, sizes["gy"], sizes["gx"]),
        mesh=mesh,
        in_specs=(cells, cells, cells, plane, P(), plane, plane),
        out_specs=(cells, plane),
        check_vma=False,
    )
```

```python
import functools

import jax
import jax.numpy as jnp
from jax import lax
from jax.experimental import pallas as pl
from jax.experimental.pallas import tpu as pltpu
from jax.sharding import PartitionSpec as P

TSTEPS = 2
ITERS = 3
K = 8
R, C = 128, 256
RE, CE = R + 16, C + 128
HALO = 5
MESH = pl.DeviceIdType.MESH
TR, EA, NO, SF, HE, CO = 0, K, 2 * K, 3 * K, 3 * K + 1, 3 * K + 2
NF = 3 * K + 2


def lane_plan():
    first, last = [], []
    for plan, widths in ((first, (5, 4, 4)), (last, (5, 5, 4))):
        lane = 0
        for base, width in zip((TR, EA, NO), widths):
            for k in range(K):
                plan.append((base + k, width, lane))
                lane += width
        for field, width in ((SF, 3), (HE, 3), (CO, 5)):
            plan.append((field, width, lane))
            lane += width
        assert lane <= 128
    return first, last


FIRST, LAST = lane_plan()


def up(now, nxt, sub):
    return pltpu.roll(jnp.where(sub == 0, nxt, now), 7, 0)


def down(now, prv, sub):
    return pltpu.roll(jnp.where(sub == 7, prv, now), 1, 0)


def east(a):
    return pltpu.roll(a, CE - 1, 1)


def west(a):
    return pltpu.roll(a, 1, 1)


def kernel(
    ngy, ngx,
    tr_hbm, ea_hbm, no_hbm, co_hbm, th_hbm, sf_hbm, he_hbm,
    tr_out, h_out,
    th, a, ci, c1, pw, pe, re, rw, me_s, mn_s, f_s, inv_s, v1_s, v2_s, row, b1, b2,
    load_sem, send_sem, recv_sem, rs_sem, rr_sem,
):
    gy, gx = lax.axis_index("gy"), lax.axis_index("gx")
    north, south = lax.rem(gy + 1, ngy), lax.rem(gy + ngy - 1, ngy)
    e_id, w_id = lax.rem(gx + 1, ngx), lax.rem(gx + ngx - 1, ngx)
    hi, z = lax.div(gx, 8), lax.rem(gx, 8)
    group1 = [
        (lax.rem(gy + dy, ngy), lax.rem(gx + 8 * dh, ngx))
        for dh in range(2) for dy in range(16) if dy or dh
    ]
    group2 = [(gy, hi * 8 + lax.rem(z + dz, 8)) for dz in range(1, 8)]
    near = [(north, gx), (south, gx), (gy, e_id), (gy, w_id),
            (north, e_id), (north, w_id), (south, e_id), (south, w_id)]

    barrier = pltpu.get_barrier_semaphore()
    for y, x in near + group1 + group2:
        pl.semaphore_signal(barrier, inc=1, device_id={"gy": y, "gx": x}, device_id_type=MESH)

    own = (pl.ds(8, R), pl.ds(0, C))
    loads = [
        pltpu.make_async_copy(src, dst, load_sem.at[i])
        for i, (src, dst) in enumerate((
            (tr_hbm, a.at[(pl.ds(TR, K),) + own]),
            (ea_hbm, a.at[(pl.ds(EA, K),) + own]),
            (no_hbm, a.at[(pl.ds(NO, K),) + own]),
            (sf_hbm, a.at[(SF,) + own]),
            (he_hbm, a.at[(HE,) + own]),
            (co_hbm, ci.at[own]),
            (th_hbm, th),
        ))
    ]
    for copy in loads:
        copy.start()
    for copy in loads:
        copy.wait()

    lane = lax.broadcasted_iota(jnp.int32, (R, 128), 1)

    def edge(field, side):
        cols = pl.ds(0 if side == 0 else C - 128, 128)
        if field == CO:
            return ci[pl.ds(8, R), cols].astype(jnp.float32)
        return a[field, pl.ds(8, R), cols]

    for side, plan, dest in ((0, FIRST, pw), (1, LAST, pe)):
        tile = jnp.zeros((R, 128), jnp.float32)
        for field, width, at in plan:
            start = 0 if side == 0 else 128 - width
            value = edge(field, side)
            shift = (at - start) % 128
            if shift:
                value = pltpu.roll(value, shift, 1)
            tile = jnp.where((lane >= at) & (lane < at + width), value, tile)
        dest[...] = tile

    pl.semaphore_wait(barrier, len(near) + len(group1) + len(group2))

    top, bottom = pl.ds(R + 3, HALO), pl.ds(8, HALO)
    ghost_s, ghost_n = pl.ds(3, HALO), pl.ds(R + 8, HALO)
    cols = pl.ds(0, C)
    every = pl.ds(0, NF)
    routes = [
        (pe, rw.at[pl.ds(8, R)], (gy, e_id)),
        (pw, re.at[pl.ds(8, R)], (gy, w_id)),
        (a.at[every, top, cols], a.at[every, ghost_s, cols], (north, gx)),
        (a.at[every, bottom, cols], a.at[every, ghost_n, cols], (south, gx)),
        (ci.at[top, cols], ci.at[ghost_s, cols], (north, gx)),
        (ci.at[bottom, cols], ci.at[ghost_n, cols], (south, gx)),
        (pe.at[pl.ds(R - HALO, HALO)], rw.at[ghost_s], (north, e_id)),
        (pw.at[pl.ds(R - HALO, HALO)], re.at[ghost_s], (north, w_id)),
        (pe.at[pl.ds(0, HALO)], rw.at[ghost_n], (south, e_id)),
        (pw.at[pl.ds(0, HALO)], re.at[ghost_n], (south, w_id)),
    ]
    sends = [
        pltpu.make_async_remote_copy(
            src_ref=src, dst_ref=dst, send_sem=send_sem.at[i], recv_sem=recv_sem.at[i],
            device_id={"gy": y, "gx": x}, device_id_type=MESH,
        )
        for i, (src, dst, (y, x)) in enumerate(routes)
    ]
    for copy in sends:
        copy.start()
    for copy in sends:
        copy.wait_recv()

    lane_e = lax.broadcasted_iota(jnp.int32, (RE, 128), 1)
    last_at = {field: (width, at) for field, width, at in LAST}
    ghost = pl.ds(C, 128)
    for field, width, at in FIRST:
        from_east = re[...]
        if at:
            from_east = pltpu.roll(from_east, 128 - at, 1)
        wide, at_w = last_at[field]
        shift = (128 - wide - at_w) % 128
        from_west = rw[...]
        if shift:
            from_west = pltpu.roll(from_west, shift, 1)
        value = jnp.where(lane_e < 64, from_east, from_west)
        a[field, :, ghost] = value
    a[CO, :, cols] = ci[:, cols].astype(jnp.float32)
    zero8 = jnp.zeros((8, CE), jnp.float32)

    @pl.when(gy == 0)
    def _():
        a[CO, pl.ds(0, 8), :] = zero8

    @pl.when(gy == ngy - 1)
    def _():
        a[CO, pl.ds(R + 8, 8), :] = zero8

    sub = lax.broadcasted_iota(jnp.int32, (8, CE), 0)
    tiles = RE // 8

    def rows(t):
        return pl.ds(8 * t, 8)

    for t in range(tiles):
        depth = a[CO, rows(t), :]
        above = a[CO, rows(min(t + 1, tiles - 1)), :]
        me_s[rows(t), :] = jnp.minimum(depth, east(depth))
        mn_s[rows(t), :] = jnp.minimum(depth, up(depth, above, sub))
        f_s[rows(t), :] = a[SF, rows(t), :]
        inv_s[rows(t), :] = 1.0 / (6.0 + a[HE, rows(t), :])

    def level(k, carry):
        kf = k.astype(jnp.float32)
        weight = th[k]

        def step(load, store):
            now = load(0)
            south_flux = jnp.zeros((8, CE), jnp.float32)
            for t in range(tiles):
                nxt = load(t + 1) if t + 1 < tiles else now
                es = jnp.where(me_s[rows(t), :] > kf, a[EA + k, rows(t), :], 0.0)
                ns = jnp.where(mn_s[rows(t), :] > kf, a[NO + k, rows(t), :], 0.0)
                fe = es * jnp.where(es > 0.0, now, east(now))
                fn = ns * jnp.where(ns > 0.0, now, up(now, nxt, sub))
                store(t, now - (fe - west(fe) + fn - down(fn, south_flux, sub)))
                now, south_flux = nxt, fn

        def put1(t, value):
            c1[rows(t), :] = value

        def put2(t, value):
            if 0 < t < tiles - 1:
                tr_out[k, pl.ds(8 * t - 8, 8), :] = value[:, :C]
            f_s[rows(t), :] += jnp.where(a[CO, rows(t), :] > kf, weight * value, 0.0)

        step(lambda t: a[TR + k, rows(t), :], put1)
        step(lambda t: c1[rows(t), :], put2)
        return carry

    lax.fori_loop(0, K, level, 0)

    nu = [jnp.zeros((8, C), jnp.float32) for _ in range(6)]
    for t in range(tiles):
        forcing = f_s[rows(t), :]
        z0 = forcing * inv_s[rows(t), :]
        if 0 < t < tiles - 1:
            nu[0] += (forcing * z0)[:, :C]
        c1[rows(t), :] = z0
        mn_s[rows(t), :] = jnp.where(a[CO, rows(t), :] > 0.0, 1.0, 0.0)

    def operator(src, store):
        def part(t):
            wet = mn_s[rows(t), :]
            w = wet * src[rows(t), :]
            h = west(w) + east(w)
            return wet, h, w + 0.5 * h

        wet, h, s = part(0)
        before = jnp.zeros_like(s)
        for t in range(tiles):
            after = part(t + 1) if t + 1 < tiles else (wet, h, s)
            store(t, wet * (h + up(s, after[2], sub) + down(s, before, sub)))
            before = s
            wet, h, s = after

    def store1(t, u):
        v = u * inv_s[rows(t), :]
        v1_s[rows(t), :] = v
        if 0 < t < tiles - 1:
            nu[1] += (v * f_s[rows(t), :])[:, :C]
            nu[2] += (v * u)[:, :C]

    def store2(t, u):
        v = u * inv_s[rows(t), :]
        v2_s[rows(t), :] = v
        if 0 < t < tiles - 1:
            nu[3] += (v1_s[rows(t), :] * u)[:, :C]
            nu[4] += (v * u)[:, :C]

    def store3(t, u):
        if 0 < t < tiles - 1:
            nu[5] += (v2_s[rows(t), :] * u)[:, :C]

    operator(c1, store1)
    operator(v1_s, store2)
    operator(v2_s, store3)

    lane1 = lax.broadcasted_iota(jnp.int32, (1, 128), 1)
    packed = jnp.zeros((1, 128), jnp.float32)
    for i, part in enumerate(nu):
        lanes = jnp.sum(part[:, :128] + part[:, 128:], axis=0, keepdims=True)
        total = jnp.sum(lanes, axis=1, keepdims=True)
        packed = jnp.where(lane1 == i, total, packed)

    reduce_sends = []
    for i, (group, slot, buf) in enumerate(((group1, gy * 2 + hi, b1), (group2, z, b2))):
        row[i] = packed
        n = len(group)
        for y, x in group:
            copy = pltpu.make_async_remote_copy(
                src_ref=row.at[i], dst_ref=buf.at[slot], send_sem=rs_sem.at[i], recv_sem=rr_sem.at[i],
                device_id={"gy": y, "gx": x}, device_id_type=MESH,
            )
            copy.start()
        buf[slot] = packed
        pltpu.make_async_copy(buf.at[pl.ds(0, n)], buf.at[pl.ds(0, n)], rr_sem.at[i]).wait()
        reduce_sends.append((buf, n, i))
        packed = jnp.sum(buf[...], axis=0)

    m = [jnp.sum(jnp.where(lane1 == i, packed, 0.0), axis=1, keepdims=True) for i in range(6)]

    def form(p, moments):
        total = None
        for i, pi in enumerate(p):
            for j, pj in enumerate(p[i:], i):
                term = (pi * pj if i == j else 2.0 * pi * pj) * moments[i + j]
                total = term if total is None else total + term
        return total

    diff = [m[i] - m[i + 1] for i in range(5)]
    one = jnp.ones_like(m[0])
    zc, pc = [one], [one]
    heights = [jnp.zeros_like(one)] * 3
    rz = m[0]
    for it in range(ITERS):
        alpha = rz / form(pc, diff)
        heights = [h + alpha * pc[i] if i < len(pc) else h for i, h in enumerate(heights)]
        if it + 1 < ITERS:
            applied = [p - q for p, q in zip(pc + [jnp.zeros_like(one)], [jnp.zeros_like(one)] + pc)]
            zc = [(zc[i] if i < len(zc) else 0.0) - alpha * applied[i] for i in range(len(applied))]
            rz_next = form(zc, m)
            beta = rz_next / rz
            pc = [zc[i] + beta * pc[i] if i < len(pc) else zc[i] for i in range(len(zc))]
            rz = rz_next

    inner = pl.ds(8, R)
    h_out[...] = heights[0] * c1[inner, cols] + heights[1] * v1_s[inner, cols] + heights[2] * v2_s[inner, cols]

    for copy in sends:
        copy.wait_send()
    for buf, n, i in reduce_sends:
        pltpu.make_async_copy(buf.at[pl.ds(0, n)], buf.at[pl.ds(0, n)], rs_sem.at[i]).wait()


def put_kernel(tr, h, tr_hbm, h_hbm, sem):
    copies = [pltpu.make_async_copy(tr, tr_hbm, sem.at[0]), pltpu.make_async_copy(h, h_hbm, sem.at[1])]
    for copy in copies:
        copy.start()
    for copy in copies:
        copy.wait()


def on_device(ngy, ngx, tracer, east_speed, north_speed, columns, thickness, surface_flux, helm):
    f32 = jnp.float32
    any_spec = pl.BlockSpec(memory_space=pltpu.HBM)
    vmem = pl.BlockSpec(memory_space=pltpu.VMEM)
    results = pl.pallas_call(
        functools.partial(kernel, ngy, ngx),
        out_shape=(pltpu.VMEM((K, R, C), f32), pltpu.VMEM((R, C), f32)),
        in_specs=[any_spec, any_spec, any_spec, any_spec, any_spec, any_spec, any_spec],
        out_specs=(vmem, vmem),
        scratch_shapes=[
            pltpu.SMEM((K,), f32),
            pltpu.VMEM((NF + 1, RE, CE), f32),
            pltpu.VMEM((RE, C), jnp.int32),
            pltpu.VMEM((RE, CE), f32),
            pltpu.VMEM((R, 128), f32),
            pltpu.VMEM((R, 128), f32),
            pltpu.VMEM((RE, 128), f32),
            pltpu.VMEM((RE, 128), f32),
        ] + [pltpu.VMEM((RE, CE), f32)] * 6 + [
            pltpu.VMEM((2, 1, 128), f32),
            pltpu.VMEM((32, 1, 128), f32),
            pltpu.VMEM((8, 1, 128), f32),
            pltpu.SemaphoreType.DMA((7,)),
            pltpu.SemaphoreType.DMA((10,)),
            pltpu.SemaphoreType.DMA((10,)),
            pltpu.SemaphoreType.DMA((2,)),
            pltpu.SemaphoreType.DMA((2,)),
        ],
        compiler_params=pltpu.CompilerParams(collective_id=0, has_side_effects=True),
    )(tracer, east_speed, north_speed, columns, thickness, surface_flux, helm)
    return pl.pallas_call(
        put_kernel,
        out_shape=(jax.ShapeDtypeStruct((K, R, C), f32), jax.ShapeDtypeStruct((R, C), f32)),
        in_specs=[vmem, vmem],
        out_specs=(any_spec, any_spec),
        scratch_shapes=[pltpu.SemaphoreType.DMA((2,))],
    )(*[pltpu.with_memory_space_constraint(r, pltpu.VMEM) for r in results])


def solution(mesh):
    sizes = mesh.shape
    cells, plane = P(None, "gy", "gx"), P("gy", "gx")
    return jax.shard_map(
        functools.partial(on_device, sizes["gy"], sizes["gx"]),
        mesh=mesh,
        in_specs=(cells, cells, cells, plane, P(), plane, plane),
        out_specs=(cells, plane),
        check_vma=False,
    )
```

```python
import functools

import jax
import jax.numpy as jnp
from jax import lax
from jax.experimental import pallas as pl
from jax.experimental.pallas import tpu as pltpu
from jax.sharding import PartitionSpec as P

ITERS = 3
K = 8
R, C, L = 128, 256, 128
RE = R + 24
HALO = 5
MESH = pl.DeviceIdType.MESH
TR, EA, NO, SF, HE, CO = 0, K, 2 * K, 3 * K, 3 * K + 1, 3 * K + 2
NF = 3 * K + 2
UNROLL = 2


def lane_plan():
    order = []
    for k in range(K):
        order += [(TR + k, 5, 5), (EA + k, 4, 5), (NO + k, 4, 4)]
    order += [(SF, 3, 3), (HE, 3, 3), (CO, 5, 5)]
    plan, at = [], 0
    for i, (field, first, last) in enumerate(order):
        if i:
            at += max(order[i - 1][1], last)
        plan.append((field, at, first, last))
    assert at + 5 <= L - 4
    return plan


PLAN = lane_plan()


def window(lane, start, width):
    start %= L
    if start + width <= L:
        return (lane >= start) & (lane < start + width)
    return (lane >= start) | (lane < start + width - L)


def turn(a, shift):
    shift %= L
    return pltpu.roll(a, shift, 1) if shift else a


def ring_east(tiles, lane):
    turned = [turn(a, -1) for a in tiles]
    if len(tiles) == 1:
        return turned
    return [jnp.where(lane < L - 1, a, turned[(i + 1) % len(tiles)]) for i, a in enumerate(turned)]


def ring_west(tiles, lane):
    turned = [turn(a, 1) for a in tiles]
    if len(tiles) == 1:
        return turned
    return [jnp.where(lane > 0, a, turned[i - 1]) for i, a in enumerate(turned)]


def rows(at):
    return pl.ds(at, 8)


def kernel(
    ngy, ngx,
    tr_hbm, ea_hbm, no_hbm, co_hbm, th_hbm, sf_hbm, he_hbm,
    tr_out, h_out,
    th, a, ci, cf, s, c1, c2, c1s, c2s, fl, fls, me_s, mn_s, mes_s, mns_s, fx, fs,
    pw, pe, re, rw, v0_s, v1_s, v2_s, sh_s, inv_s, wet_s, row, b1, b2,
    load_sem, send_sem, recv_sem, rs_sem, rr_sem,
):
    f32 = jnp.float32
    gy, gx = lax.axis_index("gy"), lax.axis_index("gx")
    north, south = lax.rem(gy + 1, ngy), lax.rem(gy + ngy - 1, ngy)
    e_id, w_id = lax.rem(gx + 1, ngx), lax.rem(gx + ngx - 1, ngx)
    hi, z = lax.div(gx, 8), lax.rem(gx, 8)
    group1 = [
        (lax.rem(gy + dy, ngy), lax.rem(gx + 8 * dh, ngx))
        for dh in range(2) for dy in range(16) if dy or dh
    ]
    group2 = [(gy, hi * 8 + lax.rem(z + dz, 8)) for dz in range(1, 8)]
    near = [(north, gx), (south, gx), (gy, e_id), (gy, w_id),
            (north, e_id), (north, w_id), (south, e_id), (south, w_id)]

    own = pl.ds(8, R)
    halves = [pl.ds(0, L), pl.ds(L, L)]
    n_load = 0

    def load(src, dst):
        nonlocal n_load
        copy = pltpu.make_async_copy(src, dst, load_sem.at[n_load])
        n_load += 1
        copy.start()
        return copy

    level_loads = []
    for k in range(K):
        level_loads.append([
            load(src.at[k, :, half], a.at[base + k, i, own])
            for src, base in ((tr_hbm, TR), (ea_hbm, EA), (no_hbm, NO))
            for i, half in enumerate(halves)
        ])
    plane_loads = [
        load(src.at[:, half], dst.at[i, own])
        for src, dst in ((sf_hbm, a.at[SF]), (he_hbm, a.at[HE]), (co_hbm, ci))
        for i, half in enumerate(halves)
    ]
    th_load = load(th_hbm, th)

    barrier = pltpu.get_barrier_semaphore()
    for y, x in near + group1 + group2:
        pl.semaphore_signal(barrier, inc=1, device_id={"gy": y, "gx": x}, device_id_type=MESH)

    lane = lax.broadcasted_iota(jnp.int32, (8, L), 1)
    tiles = range(R // 8)

    packs = [[jnp.zeros((8, L), f32) for _ in tiles] for _ in range(2)]
    for group in range(K + 1):
        for copy in level_loads[group] if group < K else plane_loads:
            copy.wait()
        for field, at, first, last in PLAN[3 * group : 3 * group + 3]:
            for side in range(2):
                width = last if side else first
                start = at - 8 - width if side else at
                mask = window(lane, start, width)
                shift = at - 8 if side else at
                for t in tiles:
                    if field == CO:
                        value = ci[side, rows(8 + 8 * t), :].astype(f32)
                    else:
                        value = a[field, side, rows(8 + 8 * t), :]
                    packs[side][t] = jnp.where(mask, turn(value, shift), packs[side][t])
    for side, dest in enumerate((pw, pe)):
        for t in tiles:
            dest[rows(8 * t), :] = packs[side][t]

    pl.semaphore_wait(barrier, len(near) + len(group1) + len(group2))

    top, bottom = pl.ds(R + 3, HALO), pl.ds(8, HALO)
    ghost_s, ghost_n = pl.ds(3, HALO), pl.ds(R + 8, HALO)
    every, both = pl.ds(0, NF), pl.ds(0, 2)
    routes = [
        (pe, rw.at[own], (gy, e_id)),
        (pw, re.at[own], (gy, w_id)),
        (a.at[every, both, top], a.at[every, both, ghost_s], (north, gx)),
        (a.at[every, both, bottom], a.at[every, both, ghost_n], (south, gx)),
        (ci.at[both, top], ci.at[both, ghost_s], (north, gx)),
        (ci.at[both, bottom], ci.at[both, ghost_n], (south, gx)),
        (pe.at[pl.ds(R - HALO, HALO)], rw.at[ghost_s], (north, e_id)),
        (pw.at[pl.ds(R - HALO, HALO)], re.at[ghost_s], (north, w_id)),
        (pe.at[pl.ds(0, HALO)], rw.at[ghost_n], (south, e_id)),
        (pw.at[pl.ds(0, HALO)], re.at[ghost_n], (south, w_id)),
    ]
    sends = [
        pltpu.make_async_remote_copy(
            src_ref=src, dst_ref=dst, send_sem=send_sem.at[i], recv_sem=recv_sem.at[i],
            device_id={"gy": y, "gx": x}, device_id_type=MESH,
        )
        for i, (src, dst, (y, x)) in enumerate(routes)
    ]
    for copy in sends:
        copy.start()
    th_load.wait()

    def seam(field, at):
        left, right = (cf[0, rows(at), :], cf[1, rows(at), :]) if field == CO else (
            a[field, 0, rows(at), :], a[field, 1, rows(at), :])
        return jnp.where(lane < 64, turn(right, 4), turn(left, -4))

    for i in range(2):
        for t in tiles:
            at = 8 + 8 * t
            cf[i, rows(at), :] = ci[i, rows(at), :].astype(f32)
            fx[i, rows(at), :] = a[SF, i, rows(at), :]
    for field in range(NF + 1):
        for t in tiles:
            s[field, rows(8 + 8 * t), :] = seam(field, 8 + 8 * t)

    def face_masks(at, below):
        depth = [cf[i, rows(at), :] for i in range(2)]
        for i, other in enumerate(ring_east(depth, lane)):
            me_s[i, rows(at), :] = jnp.minimum(depth[i], other)
            mn_s[i, rows(below), :] = jnp.minimum(cf[i, rows(below), :], cf[i, rows(below + 1), :])

    for t in tiles:
        face_masks(8 + 8 * t, min(8 + 8 * t, R - 1))

    def north_flux(k, kf, i, current, at):
        speed = jnp.where(mn_s[i, rows(at), :] > kf, a[NO + k, i, rows(at), :], 0.0)
        return speed * jnp.where(speed > 0.0, current(i, at), current(i, at + 1))

    def east_flux(k, kf, now, at):
        out = []
        for i, other in enumerate(ring_east(now, lane)):
            speed = jnp.where(me_s[i, rows(at), :] > kf, a[EA + k, i, rows(at), :], 0.0)
            out.append(speed * jnp.where(speed > 0.0, now[i], other))
        return out

    def own_step(k, kf, current, store, starts, direct):
        if not direct:
            for at in [at - 1 for at in starts] + [starts[-1]]:
                for i in range(2):
                    fl[i, rows(at), :] = north_flux(k, kf, i, current, at)
        for at in starts:
            now = [current(i, at) for i in range(2)]
            fe = east_flux(k, kf, now, at)
            fw = ring_west(fe, lane)
            for i in range(2):
                if direct:
                    fn, fb = north_flux(k, kf, i, current, at), north_flux(k, kf, i, current, at - 1)
                else:
                    fn, fb = fl[i, rows(at), :], fl[i, rows(at - 1), :]
                store(i, at, now[i] - (fe[i] - fw[i] + fn - fb))

    def own_levels(k, starts1, starts2, direct):
        kf = k.astype(f32)
        weight = th[k]

        def put1(i, at, value):
            c1[k, i, rows(at), :] = value

        def put2(i, at, value):
            c2[k, i, rows(at), :] = value
            fx[i, rows(at), :] += jnp.where(cf[i, rows(at), :] > kf, weight * value, 0.0)

        own_step(k, kf, lambda i, at: a[TR + k, i, rows(at), :], put1, starts1, direct)
        own_step(k, kf, lambda i, at: c1[k, i, rows(at), :], put2, starts2, direct)

    starts1 = [9 + 8 * t for t in range(15)] + [R - 1]
    starts2 = [12 + 8 * t for t in range(15)]

    def interior(k, carry):
        own_levels(k, starts1, starts2, False)
        return carry

    lax.fori_loop(0, K, interior, 0)

    for copy in sends:
        copy.wait_recv()

    ghosts = window(lane, 4, HALO) | window(lane, 119, HALO)
    ends = (0, R + 8)
    for at in ends:
        for i in range(2):
            cf[i, rows(at), :] = ci[i, rows(at), :].astype(f32)
    zero8 = jnp.zeros((8, L), f32)

    for at0, edge in ((0, 0), (R + 8, ngy - 1)):

        @pl.when(gy == edge)
        def _(at0=at0):
            cf[0, rows(at0), :] = zero8
            cf[1, rows(at0), :] = zero8

    for field in range(NF + 1):
        for at in ends:
            s[field, rows(at), :] = seam(field, at)
    for first_row in (0, 48, 96):
        spots = [first_row + 8 * t for t in range(6)]
        from_east = [re[rows(at), :] for at in spots]
        from_west = [rw[rows(at), :] for at in spots]
        for field, at, first, _ in PLAN:
            mask = window(lane, at, first)
            for j, spot in enumerate(spots):
                value = turn(jnp.where(mask, from_east[j], from_west[j]), 4 - at)
                s[field, rows(spot), :] = jnp.where(ghosts, value, s[field, rows(spot), :])
    for at0, edge in ((0, 0), (R + 8, ngy - 1)):

        @pl.when(gy == edge)
        def _(at0=at0):
            s[CO, rows(at0), :] = zero8

    strips = (4, R + 4)
    for at in strips:
        face_masks(at, at - 1)
        for i in range(2):
            below = at + 1
            mn_s[i, rows(below), :] = jnp.minimum(cf[i, rows(below), :], cf[i, rows(below + 1), :])
            fx[i, rows(at), :] = a[SF, i, rows(at), :]
    seam_rows = [4 + 8 * t for t in range(17)]
    below_rows = [at - 1 for at in seam_rows] + [R + 11]
    for at in seam_rows:
        depth = s[CO, rows(at), :]
        mes_s[rows(at), :] = jnp.minimum(depth, turn(depth, -1))
        fs[rows(at), :] = s[SF, rows(at), :]
    for at in below_rows:
        mns_s[rows(at), :] = jnp.minimum(s[CO, rows(at), :], s[CO, rows(at + 1), :])

    def seam_step(k, j, kf, current, store):
        for at in below_rows:
            speed = jnp.where(mns_s[rows(at), :] > kf, s[NO + k, rows(at), :], 0.0)
            fls[j, rows(at), :] = speed * jnp.where(speed > 0.0, current(at), current(at + 1))
        for at in seam_rows:
            now = current(at)
            speed = jnp.where(mes_s[rows(at), :] > kf, s[EA + k, rows(at), :], 0.0)
            fe = speed * jnp.where(speed > 0.0, now, turn(now, -1))
            store(at, now - (fe - turn(fe, 1) + fls[j, rows(at), :] - fls[j, rows(at - 1), :]))

    def edges(step, carry):
        for j in range(UNROLL):
            k = step * UNROLL + j
            kf = k.astype(f32)
            weight = th[k]

            def put1(at, value, k=k):
                c1s[k, rows(at), :] = value

            def put2(at, value, k=k, kf=kf, weight=weight):
                c2s[k, rows(at), :] = value
                fs[rows(at), :] += jnp.where(s[CO, rows(at), :] > kf, weight * value, 0.0)

            seam_step(k, j, kf, lambda at, k=k: s[TR + k, rows(at), :], put1)
            seam_step(k, j, kf, lambda at, k=k: c1s[k, rows(at), :], put2)
            own_levels(k, strips, strips, True)
        return carry

    lax.fori_loop(0, K // UNROLL, edges, 0)

    blocks = [1] + [8 * t for t in range(1, 18)]
    inside = [8 * t for t in range(1, 17)]

    def beside(tile):
        return turn(tile, 4), turn(tile, -4)

    for at in blocks:
        f_w, f_e = beside(fs[rows(at), :])
        forcing = [
            jnp.where(lane < 2, f_w, fx[0, rows(at), :]),
            jnp.where(lane >= L - 2, f_e, fx[1, rows(at), :]),
            jnp.where(lane < 64, f_e, f_w),
        ]
        helm_w, helm_e = beside(s[HE, rows(at), :])
        helm = [a[HE, 0, rows(at), :], a[HE, 1, rows(at), :], jnp.where(lane < 64, helm_e, helm_w)]
        deep_w, deep_e = beside(s[CO, rows(at), :])
        deep = [cf[0, rows(at), :], cf[1, rows(at), :], jnp.where(lane < 64, deep_e, deep_w)]
        for i in range(3):
            inv = 1.0 / (6.0 + helm[i])
            inv_s[i, rows(at), :] = inv
            wet_s[i, rows(at), :] = jnp.where(deep[i] > 0.0, 1.0, 0.0)
            fx[i, rows(at), :] = forcing[i]
            v0_s[i, rows(at), :] = forcing[i] * inv

    nu = [[jnp.zeros((8, L), f32) for _ in range(2)] for _ in range(6)]

    def operator(n, src, spots, store):
        spread = {}
        for at in blocks:
            w = [src[i, rows(at), :] for i in range(3)]
            if n == 0:
                w = [wet_s[i, rows(at), :] * w[i] for i in range(3)]
            h = [x + y for x, y in zip(ring_west(w, lane), ring_east(w, lane))]
            spread[at] = h
            for i in range(3):
                sh_s[n, i, rows(at), :] = w[i] + 0.5 * h[i]
        for at in spots:
            for i in range(3):
                u = wet_s[i, rows(at), :] * (
                    spread[at][i] + sh_s[n, i, rows(at + 1), :] + sh_s[n, i, rows(at - 1), :])
                store(i, at, u)

    def counted(i, at):
        return i < 2 and at in inside

    def store1(i, at, u):
        v = u * inv_s[i, rows(at), :]
        v1_s[i, rows(at), :] = v
        if counted(i, at):
            f = fx[i, rows(at), :]
            nu[0][i] += f * v0_s[i, rows(at), :]
            nu[1][i] += v * f
            nu[2][i] += v * u

    def store2(i, at, u):
        v = u * inv_s[i, rows(at), :]
        v2_s[i, rows(at), :] = v
        if counted(i, at):
            nu[3][i] += v1_s[i, rows(at), :] * u
            nu[4][i] += v * u

    def store3(i, at, u):
        if counted(i, at):
            nu[5][i] += v2_s[i, rows(at), :] * u

    operator(0, v0_s, blocks, store1)
    operator(1, v1_s, blocks, store2)
    operator(2, v2_s, inside, store3)

    def finish_tracer():
        def put(k, carry):
            for t in tiles:
                at = 8 + 8 * t
                turned = beside(c2s[k, rows(at), :])
                for i, mask in enumerate((lane < 2, lane >= L - 2)):
                    tr_out[k, rows(8 * t), halves[i]] = jnp.where(mask, turned[i], c2[k, i, rows(at), :])
            return carry

        lax.fori_loop(0, K, put, 0)

    lane1 = lax.broadcasted_iota(jnp.int32, (1, 128), 1)
    packed = jnp.zeros((1, 128), jnp.float32)
    for i, part in enumerate(nu):
        lanes = jnp.sum(part[0] + part[1], axis=0, keepdims=True)
        total = jnp.sum(lanes, axis=1, keepdims=True)
        packed = jnp.where(lane1 == i, total, packed)

    reduce_sends = []
    for i, (group, slot, buf) in enumerate(((group1, gy * 2 + hi, b1), (group2, z, b2))):
        row[i] = packed
        n = len(group)
        for y, x in group:
            copy = pltpu.make_async_remote_copy(
                src_ref=row.at[i], dst_ref=buf.at[slot], send_sem=rs_sem.at[i], recv_sem=rr_sem.at[i],
                device_id={"gy": y, "gx": x}, device_id_type=MESH,
            )
            copy.start()
        buf[slot] = packed
        if i == 0:
            finish_tracer()
        pltpu.make_async_copy(buf.at[pl.ds(0, n)], buf.at[pl.ds(0, n)], rr_sem.at[i]).wait()
        reduce_sends.append((buf, n, i))
        packed = jnp.sum(buf[...], axis=0)

    m = [jnp.sum(jnp.where(lane1 == i, packed, 0.0), axis=1, keepdims=True) for i in range(6)]

    def form(p, moments):
        total = None
        for i, pi in enumerate(p):
            for j, pj in enumerate(p[i:], i):
                term = (pi * pj if i == j else 2.0 * pi * pj) * moments[i + j]
                total = term if total is None else total + term
        return total

    diff = [m[i] - m[i + 1] for i in range(5)]
    one = jnp.ones_like(m[0])
    zc, pc = [one], [one]
    heights = [jnp.zeros_like(one)] * 3
    rz = m[0]
    for it in range(ITERS):
        alpha = rz / form(pc, diff)
        heights = [h + alpha * pc[i] if i < len(pc) else h for i, h in enumerate(heights)]
        if it + 1 < ITERS:
            applied = [p - q for p, q in zip(pc + [jnp.zeros_like(one)], [jnp.zeros_like(one)] + pc)]
            zc = [(zc[i] if i < len(zc) else 0.0) - alpha * applied[i] for i in range(len(applied))]
            rz_next = form(zc, m)
            beta = rz_next / rz
            pc = [zc[i] + beta * pc[i] if i < len(pc) else zc[i] for i in range(len(zc))]
            rz = rz_next

    for t in tiles:
        at = 8 + 8 * t
        for i in range(2):
            h_out[rows(8 * t), halves[i]] = (
                heights[0] * v0_s[i, rows(at), :] + heights[1] * v1_s[i, rows(at), :] + heights[2] * v2_s[i, rows(at), :])

    for copy in sends:
        copy.wait_send()
    for buf, n, i in reduce_sends:
        pltpu.make_async_copy(buf.at[pl.ds(0, n)], buf.at[pl.ds(0, n)], rs_sem.at[i]).wait()


def put_kernel(tr, h, tr_hbm, h_hbm, sem):
    copies = [pltpu.make_async_copy(tr, tr_hbm, sem.at[0]), pltpu.make_async_copy(h, h_hbm, sem.at[1])]
    for copy in copies:
        copy.start()
    for copy in copies:
        copy.wait()


def on_device(ngy, ngx, tracer, east_speed, north_speed, columns, thickness, surface_flux, helm):
    f32 = jnp.float32
    any_spec = pl.BlockSpec(memory_space=pltpu.HBM)
    vmem = pl.BlockSpec(memory_space=pltpu.VMEM)
    results = pl.pallas_call(
        functools.partial(kernel, ngy, ngx),
        out_shape=(pltpu.VMEM((K, R, C), f32), pltpu.VMEM((R, C), f32)),
        in_specs=[any_spec, any_spec, any_spec, any_spec, any_spec, any_spec, any_spec],
        out_specs=(vmem, vmem),
        scratch_shapes=[
            pltpu.SMEM((K,), f32),
            pltpu.VMEM((NF, 2, RE, L), f32),
            pltpu.VMEM((2, RE, L), jnp.int32),
            pltpu.VMEM((2, RE, L), f32),
            pltpu.VMEM((NF + 1, RE, L), f32),
            pltpu.VMEM((K, 2, RE, L), f32),
            pltpu.VMEM((K, 2, RE, L), f32),
            pltpu.VMEM((K, RE, L), f32),
            pltpu.VMEM((K, RE, L), f32),
            pltpu.VMEM((2, RE, L), f32),
            pltpu.VMEM((UNROLL, RE, L), f32),
            pltpu.VMEM((2, RE, L), f32),
            pltpu.VMEM((2, RE, L), f32),
            pltpu.VMEM((RE, L), f32),
            pltpu.VMEM((RE, L), f32),
            pltpu.VMEM((3, RE, L), f32),
            pltpu.VMEM((RE, L), f32),
            pltpu.VMEM((R, L), f32),
            pltpu.VMEM((R, L), f32),
            pltpu.VMEM((RE, L), f32),
            pltpu.VMEM((RE, L), f32),
            pltpu.VMEM((3, RE, L), f32),
            pltpu.VMEM((3, RE, L), f32),
            pltpu.VMEM((3, RE, L), f32),
            pltpu.VMEM((3, 3, RE, L), f32),
            pltpu.VMEM((3, RE, L), f32),
            pltpu.VMEM((3, RE, L), f32),
            pltpu.VMEM((2, 1, L), f32),
            pltpu.VMEM((32, 1, L), f32),
            pltpu.VMEM((8, 1, L), f32),
            pltpu.SemaphoreType.DMA((6 * K + 7,)),
            pltpu.SemaphoreType.DMA((10,)),
            pltpu.SemaphoreType.DMA((10,)),
            pltpu.SemaphoreType.DMA((2,)),
            pltpu.SemaphoreType.DMA((2,)),
        ],
        compiler_params=pltpu.CompilerParams(collective_id=0, has_side_effects=True),
    )(tracer, east_speed, north_speed, columns, thickness, surface_flux, helm)
    return pl.pallas_call(
        put_kernel,
        out_shape=(jax.ShapeDtypeStruct((K, R, C), f32), jax.ShapeDtypeStruct((R, C), f32)),
        in_specs=[vmem, vmem],
        out_specs=(any_spec, any_spec),
        scratch_shapes=[pltpu.SemaphoreType.DMA((2,))],
    )(*[pltpu.with_memory_space_constraint(r, pltpu.VMEM) for r in results])


def solution(mesh):
    sizes = mesh.shape
    cells, plane = P(None, "gy", "gx"), P("gy", "gx")
    return jax.shard_map(
        functools.partial(on_device, sizes["gy"], sizes["gx"]),
        mesh=mesh,
        in_specs=(cells, cells, cells, plane, P(), plane, plane),
        out_specs=(cells, plane),
        check_vma=False,
    )
```

```python
import functools

import jax
import jax.numpy as jnp
from jax import lax
from jax.experimental import pallas as pl
from jax.experimental.pallas import tpu as pltpu
from jax.sharding import PartitionSpec as P

ITERS = 3
K = 8
R, C, L = 128, 256, 128
RE = R + 32
HALO = 5
MESH = pl.DeviceIdType.MESH
TR, EA, NO, SF, HE, CO = 0, K, 2 * K, 3 * K, 3 * K + 1, 3 * K + 2
NF = 3 * K + 2
UNROLL = 4
STRIP_UNROLL = 4
PAIR = 2


def lane_plan():
    order = []
    for k in range(K):
        order += [(TR + k, 5, 5), (EA + k, 4, 5), (NO + k, 4, 4)]
    order += [(SF, 3, 3), (HE, 3, 3), (CO, 5, 5)]
    plan, at = [], 0
    for i, (field, first, last) in enumerate(order):
        if i:
            at += max(order[i - 1][1], last)
        plan.append((field, at, first, last))
    assert at + 5 <= L - 4
    return plan


PLAN = lane_plan()


def window(lane, start, width):
    start %= L
    if start + width <= L:
        return (lane >= start) & (lane < start + width)
    return (lane >= start) | (lane < start + width - L)


def turn(a, shift):
    shift %= L
    return pltpu.roll(a, shift, 1) if shift else a


def ring_east(tiles, lane):
    turned = [turn(a, -1) for a in tiles]
    if len(tiles) == 1:
        return turned
    return [jnp.where(lane < L - 1, a, turned[(i + 1) % len(tiles)]) for i, a in enumerate(turned)]


def ring_west(tiles, lane):
    turned = [turn(a, 1) for a in tiles]
    if len(tiles) == 1:
        return turned
    return [jnp.where(lane > 0, a, turned[i - 1]) for i, a in enumerate(turned)]


def rows(at):
    return pl.ds(at, 8)


def kernel(
    ngy, ngx,
    tr_hbm, ea_hbm, no_hbm, co_hbm, th_hbm, sf_hbm, he_hbm,
    tr_out, h_out,
    th, a, ci, cf, s, c1, c2, c1s, c2s, fl, fls, me_s, mn_s, mes_s, mns_s, fx, fs,
    pw, pe, re, rw, v0_s, v1_s, v2_s, sh_s, inv_s, wet_s, row, b1, b2,
    load_sem, send_sem, recv_sem, rs_sem, rr_sem,
):
    f32 = jnp.float32
    gy, gx = lax.axis_index("gy"), lax.axis_index("gx")
    north, south = lax.rem(gy + 1, ngy), lax.rem(gy + ngy - 1, ngy)
    e_id, w_id = lax.rem(gx + 1, ngx), lax.rem(gx + ngx - 1, ngx)
    hi, z = lax.div(gx, 8), lax.rem(gx, 8)
    group1 = [
        (lax.rem(gy + dy, ngy), lax.rem(gx + 8 * dh, ngx))
        for dh in range(2) for dy in range(16) if dy or dh
    ]
    far1 = [device for i, device in enumerate(group1) if i not in (0, 14)]
    group2 = [(gy, hi * 8 + lax.rem(z + dz, 8)) for dz in range(1, 8)]
    near = [(north, gx), (south, gx), (gy, e_id), (gy, w_id),
            (north, e_id), (north, w_id), (south, e_id), (south, w_id)]

    barrier = pltpu.get_barrier_semaphore()

    def greet(devices):
        for y, x in devices:
            pl.semaphore_signal(barrier, inc=1, device_id={"gy": y, "gx": x}, device_id_type=MESH)

    greet(near)
    own, both = pl.ds(8, R), pl.ds(0, 2)
    halves = [pl.ds(0, L), pl.ds(L, L)]
    for g in range(K // PAIR):
        for src, base in ((tr_hbm, TR), (ea_hbm, EA), (no_hbm, NO)):
            for i, half in enumerate(halves):
                pltpu.make_async_copy(
                    src.at[pl.ds(PAIR * g, PAIR), :, half], a.at[pl.ds(base + PAIR * g, PAIR), i, own], load_sem.at[g]
                ).start()
    for src, dst in ((sf_hbm, a.at[SF]), (he_hbm, a.at[HE]), (co_hbm, ci)):
        for i, half in enumerate(halves):
            pltpu.make_async_copy(src.at[:, half], dst.at[i, own], load_sem.at[K // PAIR]).start()
    th_load = pltpu.make_async_copy(th_hbm, th, load_sem.at[K // PAIR + 1])
    th_load.start()
    greet(far1 + group2)

    def wait_rows(ref, sem):
        pltpu.make_async_copy(ref, ref, sem).wait()

    lane = lax.broadcasted_iota(jnp.int32, (8, L), 1)
    tiles = range(R // 8)

    packs = [[jnp.zeros((8, L), f32) for _ in tiles] for _ in range(2)]
    for g in range(K // PAIR + 1):
        wait_rows(a.at[pl.ds(0, 3 * PAIR if g < K // PAIR else 3), both, own], load_sem.at[g])
        for field, at, first, last in PLAN[3 * PAIR * g : 3 * PAIR * (g + 1)]:
            for side in range(2):
                width = last if side else first
                start = at - 8 - width if side else at
                mask = window(lane, start, width)
                shift = at - 8 if side else at
                for t in tiles:
                    if field == CO:
                        value = ci[side, rows(8 + 8 * t), :].astype(f32)
                    else:
                        value = a[field, side, rows(8 + 8 * t), :]
                    packs[side][t] = jnp.where(mask, turn(value, shift), packs[side][t])
    for side, dest in enumerate((pw, pe)):
        for t in tiles:
            dest[rows(8 * t), :] = packs[side][t]

    pl.semaphore_wait(barrier, len(near) + len(far1) + len(group2))

    top, bottom = pl.ds(R + 3, HALO), pl.ds(8, HALO)
    ghost_s, ghost_n = pl.ds(3, HALO), pl.ds(R + 8, HALO)
    every = pl.ds(0, NF)
    routes = [
        (0, pe.at[pl.ds(R - HALO, HALO)], rw.at[ghost_s], (north, e_id)),
        (0, pw.at[pl.ds(R - HALO, HALO)], re.at[ghost_s], (north, w_id)),
        (0, pe.at[pl.ds(0, HALO)], rw.at[ghost_n], (south, e_id)),
        (0, pw.at[pl.ds(0, HALO)], re.at[ghost_n], (south, w_id)),
        (0, pe, rw.at[own], (gy, e_id)),
        (0, pw, re.at[own], (gy, w_id)),
        (1, ci.at[both, top], ci.at[both, ghost_s], (north, gx)),
        (1, ci.at[both, bottom], ci.at[both, ghost_n], (south, gx)),
        (1, a.at[every, both, top], a.at[every, both, ghost_s], (north, gx)),
        (1, a.at[every, both, bottom], a.at[every, both, ghost_n], (south, gx)),
    ]
    for kind, src, dst, (y, x) in routes:
        pltpu.make_async_remote_copy(
            src_ref=src, dst_ref=dst, send_sem=send_sem, recv_sem=recv_sem.at[kind],
            device_id={"gy": y, "gx": x}, device_id_type=MESH,
        ).start()
    column_rows = (1, 2, R + 2 * HALO)
    row_rows = (2, 2, 5 * (NF + 1))
    sent_rows = (3, 2, 136)
    assert 2 * (R + 2 * HALO) == 2 * R + 4 * HALO and 4 * 5 * (NF + 1) == 2 * 2 * HALO * (NF + 1)
    assert 6 * 136 == 2 * (R + 2 * HALO) + 20 * (NF + 1)

    def sized(shape):
        return c1.at[pl.ds(0, shape[0]), pl.ds(0, shape[1]), pl.ds(0, shape[2])]

    th_load.wait()

    def seam(field, at):
        left, right = (cf[0, rows(at), :], cf[1, rows(at), :]) if field == CO else (
            a[field, 0, rows(at), :], a[field, 1, rows(at), :])
        return jnp.where(lane < 64, turn(right, 4), turn(left, -4))

    def diagonal(i, at, helm, depth):
        inv_s[i, rows(at), :] = 1.0 / (6.0 + helm)
        wet_s[i, rows(at), :] = jnp.where(depth > 0.0, 1.0, 0.0)

    for i in range(2):
        for t in tiles:
            at = 8 + 8 * t
            cf[i, rows(at), :] = ci[i, rows(at), :].astype(f32)
            fx[i, rows(at), :] = a[SF, i, rows(at), :]
            diagonal(i, at, a[HE, i, rows(at), :], cf[i, rows(at), :])
    for field in range(NF + 1):
        for t in tiles:
            s[field, rows(8 + 8 * t), :] = seam(field, 8 + 8 * t)

    def face_masks(at, below):
        depth = [cf[i, rows(at), :] for i in range(2)]
        for i, other in enumerate(ring_east(depth, lane)):
            me_s[i, rows(at), :] = jnp.minimum(depth[i], other)
            mn_s[i, rows(below), :] = jnp.minimum(cf[i, rows(below), :], cf[i, rows(below + 1), :])

    for t in tiles:
        face_masks(8 + 8 * t, min(8 + 8 * t, R - 1))

    def north_flux(k, kf, i, current, at):
        speed = jnp.where(mn_s[i, rows(at), :] > kf, a[NO + k, i, rows(at), :], 0.0)
        return speed * jnp.where(speed > 0.0, current(i, at), current(i, at + 1))

    def east_flux(k, kf, now, at):
        out = []
        for i, other in enumerate(ring_east(now, lane)):
            speed = jnp.where(me_s[i, rows(at), :] > kf, a[EA + k, i, rows(at), :], 0.0)
            out.append(speed * jnp.where(speed > 0.0, now[i], other))
        return out

    def own_step(k, kf, current, store, starts, direct):
        if not direct:
            for at in [at - 1 for at in starts] + [starts[-1]]:
                for i in range(2):
                    fl[i, rows(at), :] = north_flux(k, kf, i, current, at)
        for at in starts:
            now = [current(i, at) for i in range(2)]
            fe = east_flux(k, kf, now, at)
            fw = ring_west(fe, lane)
            for i in range(2):
                if direct:
                    fn, fb = north_flux(k, kf, i, current, at), north_flux(k, kf, i, current, at - 1)
                else:
                    fn, fb = fl[i, rows(at), :], fl[i, rows(at - 1), :]
                store(i, at, now[i] - (fe[i] - fw[i] + fn - fb))

    def own_levels(k, starts1, starts2, direct):
        kf = k.astype(f32)
        weight = th[k]

        def put1(i, at, value):
            c1[k, i, rows(at), :] = value

        def put2(i, at, value):
            c2[k, i, rows(at), :] = value
            fx[i, rows(at), :] += jnp.where(cf[i, rows(at), :] > kf, weight * value, 0.0)

        own_step(k, kf, lambda i, at: a[TR + k, i, rows(at), :], put1, starts1, direct)
        own_step(k, kf, lambda i, at: c1[k, i, rows(at), :], put2, starts2, direct)

    starts1 = [9 + 8 * t for t in range(15)] + [R - 1]
    starts2 = [12 + 8 * t for t in range(15)]

    def interior(k, carry):
        own_levels(k, starts1, starts2, False)
        return carry

    lax.fori_loop(0, K, interior, 0)

    wait_rows(sized(column_rows), recv_sem.at[0])

    ghosts = window(lane, 4, HALO) | window(lane, 119, HALO)
    ends = (0, R + 8)
    for first_row in (0, 48, 96):
        spots = [first_row + 8 * t for t in range(6)]
        from_east = [re[rows(at), :] for at in spots]
        from_west = [rw[rows(at), :] for at in spots]
        for field, at, first, _ in PLAN:
            mask = window(lane, at, first)
            for j, spot in enumerate(spots):
                value = turn(jnp.where(mask, from_east[j], from_west[j]), 4 - at)
                if spot not in ends:
                    value = jnp.where(ghosts, value, s[field, rows(spot), :])
                s[field, rows(spot), :] = value

    def beside(tile):
        return turn(tile, 4), turn(tile, -4)

    def ghost_tile(field, at):
        west, east = beside(s[field, rows(at), :])
        return jnp.where(lane < 64, east, west)

    for t in tiles:
        at = 8 + 8 * t
        depth = s[CO, rows(at), :]
        mes_s[rows(at), :] = jnp.minimum(depth, turn(depth, -1))
        below = min(at, R - 1)
        mns_s[rows(below), :] = jnp.minimum(s[CO, rows(below), :], s[CO, rows(below + 1), :])
        fs[rows(at), :] = s[SF, rows(at), :]
        diagonal(2, at, ghost_tile(HE, at), ghost_tile(CO, at))

    def seam_flux(k, kf, current, at):
        speed = jnp.where(mns_s[rows(at), :] > kf, s[NO + k, rows(at), :], 0.0)
        return speed * jnp.where(speed > 0.0, current(at), current(at + 1))

    def seam_step(k, j, kf, current, store, starts, direct):
        if not direct:
            for at in [at - 1 for at in starts] + [starts[-1]]:
                fls[j, rows(at), :] = seam_flux(k, kf, current, at)
        for at in starts:
            now = current(at)
            speed = jnp.where(mes_s[rows(at), :] > kf, s[EA + k, rows(at), :], 0.0)
            fe = speed * jnp.where(speed > 0.0, now, turn(now, -1))
            if direct:
                fn, fb = seam_flux(k, kf, current, at), seam_flux(k, kf, current, at - 1)
            else:
                fn, fb = fls[j, rows(at), :], fls[j, rows(at - 1), :]
            store(at, now - (fe - turn(fe, 1) + fn - fb))

    def seam_levels(k, j, starts1, starts2, direct):
        kf = k.astype(f32)
        weight = th[k]

        def put1(at, value):
            c1s[k, rows(at), :] = value

        def put2(at, value):
            c2s[k, rows(at), :] = value
            fs[rows(at), :] += jnp.where(s[CO, rows(at), :] > kf, weight * value, 0.0)

        seam_step(k, j, kf, lambda at: s[TR + k, rows(at), :], put1, starts1, direct)
        seam_step(k, j, kf, lambda at: c1s[k, rows(at), :], put2, starts2, direct)

    def seams(step, carry):
        for j in range(UNROLL):
            seam_levels(step * UNROLL + j, j, starts1, starts2, False)
        return carry

    lax.fori_loop(0, K // UNROLL, seams, 0)

    wait_rows(sized(row_rows), recv_sem.at[1])

    zero8 = jnp.zeros((8, L), f32)
    for at in ends:
        for i in range(2):
            cf[i, rows(at), :] = ci[i, rows(at), :].astype(f32)

    def shut():
        for at0, edge in ((0, 0), (R + 8, ngy - 1)):

            @pl.when(gy == edge)
            def _(at0=at0):
                cf[0, rows(at0), :] = zero8
                cf[1, rows(at0), :] = zero8
                s[CO, rows(at0), :] = zero8

    for field in range(NF + 1):
        for at in ends:
            s[field, rows(at), :] = jnp.where(ghosts, s[field, rows(at), :], seam(field, at))
    shut()

    strips = (4, R + 4)
    for at in strips:
        face_masks(at, at - 1)
        below = at + 1
        for i in range(2):
            mn_s[i, rows(below), :] = jnp.minimum(cf[i, rows(below), :], cf[i, rows(below + 1), :])
            fx[i, rows(at), :] = a[SF, i, rows(at), :]
        depth = s[CO, rows(at), :]
        mes_s[rows(at), :] = jnp.minimum(depth, turn(depth, -1))
        for below in (at - 1, at + 1):
            mns_s[rows(below), :] = jnp.minimum(s[CO, rows(below), :], s[CO, rows(below + 1), :])
        fs[rows(at), :] = s[SF, rows(at), :]
    for at in ends:
        for i in range(2):
            diagonal(i, at, a[HE, i, rows(at), :], cf[i, rows(at), :])
        diagonal(2, at, ghost_tile(HE, at), ghost_tile(CO, at))

    def edges(step, carry):
        for j in range(STRIP_UNROLL):
            k = step * STRIP_UNROLL + j
            own_levels(k, strips, strips, True)
            seam_levels(k, j, strips, strips, True)
        return carry

    lax.fori_loop(0, K // STRIP_UNROLL, edges, 0)

    blocks = [1] + [8 * t for t in range(1, 18)]
    inside = [8 * t for t in range(1, 17)]

    for at in blocks:
        f_w, f_e = beside(fs[rows(at), :])
        forcing = [
            jnp.where(lane < 2, f_w, fx[0, rows(at), :]),
            jnp.where(lane >= L - 2, f_e, fx[1, rows(at), :]),
            jnp.where(lane < 64, f_e, f_w),
        ]
        for i in range(3):
            fx[i, rows(at), :] = forcing[i]
            v0_s[i, rows(at), :] = forcing[i] * inv_s[i, rows(at), :]

    nu = [[jnp.zeros((8, L), f32) for _ in range(2)] for _ in range(6)]

    def operator(n, src, spots, store):
        spread = {}
        for at in blocks:
            w = [src[i, rows(at), :] for i in range(3)]
            if n == 0:
                w = [wet_s[i, rows(at), :] * w[i] for i in range(3)]
            h = [x + y for x, y in zip(ring_west(w, lane), ring_east(w, lane))]
            spread[at] = h
            for i in range(3):
                sh_s[n, i, rows(at), :] = w[i] + 0.5 * h[i]
        for at in spots:
            for i in range(3):
                u = wet_s[i, rows(at), :] * (
                    spread[at][i] + sh_s[n, i, rows(at + 1), :] + sh_s[n, i, rows(at - 1), :])
                store(i, at, u)

    def counted(i, at):
        return i < 2 and at in inside

    def store1(i, at, u):
        v = u * inv_s[i, rows(at), :]
        v1_s[i, rows(at), :] = v
        if counted(i, at):
            f = fx[i, rows(at), :]
            nu[0][i] += f * v0_s[i, rows(at), :]
            nu[1][i] += v * f
            nu[2][i] += v * u

    def store2(i, at, u):
        v = u * inv_s[i, rows(at), :]
        v2_s[i, rows(at), :] = v
        if counted(i, at):
            nu[3][i] += v1_s[i, rows(at), :] * u
            nu[4][i] += v * u

    def store3(i, at, u):
        if counted(i, at):
            nu[5][i] += v2_s[i, rows(at), :] * u

    operator(0, v0_s, blocks, store1)
    operator(1, v1_s, blocks, store2)
    operator(2, v2_s, inside, store3)

    def finish_tracer():
        def put(k, carry):
            for t in tiles:
                at = 8 + 8 * t
                turned = beside(c2s[k, rows(at), :])
                for i, mask in enumerate((lane < 2, lane >= L - 2)):
                    tr_out[k, rows(8 * t), halves[i]] = jnp.where(mask, turned[i], c2[k, i, rows(at), :])
            return carry

        lax.fori_loop(0, K, put, 0)

    lane1 = lax.broadcasted_iota(jnp.int32, (1, 128), 1)
    packed = jnp.zeros((1, 128), jnp.float32)
    for i, part in enumerate(nu):
        lanes = jnp.sum(part[0] + part[1], axis=0, keepdims=True)
        total = jnp.sum(lanes, axis=1, keepdims=True)
        packed = jnp.where(lane1 == i, total, packed)

    reduce_sends = []
    for i, (group, slot, buf) in enumerate(((group1, gy * 2 + hi, b1), (group2, z, b2))):
        row[i] = packed
        n = len(group)
        for y, x in group:
            copy = pltpu.make_async_remote_copy(
                src_ref=row.at[i], dst_ref=buf.at[slot], send_sem=rs_sem.at[i], recv_sem=rr_sem.at[i],
                device_id={"gy": y, "gx": x}, device_id_type=MESH,
            )
            copy.start()
        buf[slot] = packed
        if i == 0:
            finish_tracer()
        pltpu.make_async_copy(buf.at[pl.ds(0, n)], buf.at[pl.ds(0, n)], rr_sem.at[i]).wait()
        reduce_sends.append((buf, n, i))
        packed = jnp.sum(buf[...], axis=0)

    m = [jnp.sum(jnp.where(lane1 == i, packed, 0.0), axis=1, keepdims=True) for i in range(6)]

    def form(p, moments):
        total = None
        for i, pi in enumerate(p):
            for j, pj in enumerate(p[i:], i):
                term = (pi * pj if i == j else 2.0 * pi * pj) * moments[i + j]
                total = term if total is None else total + term
        return total

    diff = [m[i] - m[i + 1] for i in range(5)]
    one = jnp.ones_like(m[0])
    zc, pc = [one], [one]
    heights = [jnp.zeros_like(one)] * 3
    rz = m[0]
    for it in range(ITERS):
        alpha = rz / form(pc, diff)
        heights = [h + alpha * pc[i] if i < len(pc) else h for i, h in enumerate(heights)]
        if it + 1 < ITERS:
            applied = [p - q for p, q in zip(pc + [jnp.zeros_like(one)], [jnp.zeros_like(one)] + pc)]
            zc = [(zc[i] if i < len(zc) else 0.0) - alpha * applied[i] for i in range(len(applied))]
            rz_next = form(zc, m)
            beta = rz_next / rz
            pc = [zc[i] + beta * pc[i] if i < len(pc) else zc[i] for i in range(len(zc))]
            rz = rz_next

    for t in tiles:
        at = 8 + 8 * t
        for i in range(2):
            h_out[rows(8 * t), halves[i]] = (
                heights[0] * v0_s[i, rows(at), :] + heights[1] * v1_s[i, rows(at), :] + heights[2] * v2_s[i, rows(at), :])

    wait_rows(sized(sent_rows), send_sem)
    for buf, n, i in reduce_sends:
        pltpu.make_async_copy(buf.at[pl.ds(0, n)], buf.at[pl.ds(0, n)], rs_sem.at[i]).wait()


def put_kernel(tr, h, tr_hbm, h_hbm, sem):
    copies = [pltpu.make_async_copy(tr, tr_hbm, sem.at[0]), pltpu.make_async_copy(h, h_hbm, sem.at[1])]
    for copy in copies:
        copy.start()
    for copy in copies:
        copy.wait()


def on_device(ngy, ngx, tracer, east_speed, north_speed, columns, thickness, surface_flux, helm):
    f32 = jnp.float32
    any_spec = pl.BlockSpec(memory_space=pltpu.HBM)
    vmem = pl.BlockSpec(memory_space=pltpu.VMEM)
    results = pl.pallas_call(
        functools.partial(kernel, ngy, ngx),
        out_shape=(pltpu.VMEM((K, R, C), f32), pltpu.VMEM((R, C), f32)),
        in_specs=[any_spec, any_spec, any_spec, any_spec, any_spec, any_spec, any_spec],
        out_specs=(vmem, vmem),
        scratch_shapes=[
            pltpu.SMEM((K,), f32),
            pltpu.VMEM((NF, 2, RE, L), f32),
            pltpu.VMEM((2, RE, L), jnp.int32),
            pltpu.VMEM((2, RE, L), f32),
            pltpu.VMEM((NF + 1, RE, L), f32),
            pltpu.VMEM((K, 2, RE, L), f32),
            pltpu.VMEM((K, 2, RE, L), f32),
            pltpu.VMEM((K, RE, L), f32),
            pltpu.VMEM((K, RE, L), f32),
            pltpu.VMEM((2, RE, L), f32),
            pltpu.VMEM((UNROLL, RE, L), f32),
            pltpu.VMEM((2, RE, L), f32),
            pltpu.VMEM((2, RE, L), f32),
            pltpu.VMEM((RE, L), f32),
            pltpu.VMEM((RE, L), f32),
            pltpu.VMEM((3, RE, L), f32),
            pltpu.VMEM((RE, L), f32),
            pltpu.VMEM((R, L), f32),
            pltpu.VMEM((R, L), f32),
            pltpu.VMEM((RE, L), f32),
            pltpu.VMEM((RE, L), f32),
            pltpu.VMEM((3, RE, L), f32),
            pltpu.VMEM((3, RE, L), f32),
            pltpu.VMEM((3, RE, L), f32),
            pltpu.VMEM((3, 3, RE, L), f32),
            pltpu.VMEM((3, RE, L), f32),
            pltpu.VMEM((3, RE, L), f32),
            pltpu.VMEM((2, 1, L), f32),
            pltpu.VMEM((32, 1, L), f32),
            pltpu.VMEM((8, 1, L), f32),
            pltpu.SemaphoreType.DMA((K // PAIR + 2,)),
            pltpu.SemaphoreType.DMA,
            pltpu.SemaphoreType.DMA((2,)),
            pltpu.SemaphoreType.DMA((2,)),
            pltpu.SemaphoreType.DMA((2,)),
        ],
        compiler_params=pltpu.CompilerParams(collective_id=0, has_side_effects=True),
    )(tracer, east_speed, north_speed, columns, thickness, surface_flux, helm)
    return pl.pallas_call(
        put_kernel,
        out_shape=(jax.ShapeDtypeStruct((K, R, C), f32), jax.ShapeDtypeStruct((R, C), f32)),
        in_specs=[vmem, vmem],
        out_specs=(any_spec, any_spec),
        scratch_shapes=[pltpu.SemaphoreType.DMA((2,))],
    )(*[pltpu.with_memory_space_constraint(r, pltpu.VMEM) for r in results])


def solution(mesh):
    sizes = mesh.shape
    cells, plane = P(None, "gy", "gx"), P("gy", "gx")
    return jax.shard_map(
        functools.partial(on_device, sizes["gy"], sizes["gx"]),
        mesh=mesh,
        in_specs=(cells, cells, cells, plane, P(), plane, plane),
        out_specs=(cells, plane),
        check_vma=False,
    )
```

```python
import functools

import jax
import jax.numpy as jnp
from jax import lax
from jax.experimental import pallas as pl
from jax.experimental.pallas import tpu as pltpu
from jax.sharding import PartitionSpec as P

ITERS = 3
K = 8
R, C, L = 128, 256, 128
RE = R + 24
HALO = 5
MESH = pl.DeviceIdType.MESH
TR, EA, NO, SF, HE, CO = 0, K, 2 * K, 3 * K, 3 * K + 1, 3 * K + 2
NF = 3 * K + 2
UNROLL = 4
STRIP_UNROLL = 8
PAIR = 2


def lane_plan():
    order = []
    for k in range(K):
        order += [(TR + k, 5, 5), (EA + k, 4, 5), (NO + k, 4, 4)]
    order += [(SF, 3, 3), (HE, 3, 3), (CO, 5, 5)]
    plan, at = [], 0
    for i, (field, first, last) in enumerate(order):
        if i:
            at += max(order[i - 1][1], last)
        plan.append((field, at, first, last))
    assert at + 5 <= L - 4
    return plan


PLAN = lane_plan()


def window(lane, start, width):
    start %= L
    if start + width <= L:
        return (lane >= start) & (lane < start + width)
    return (lane >= start) | (lane < start + width - L)


def turn(a, shift):
    shift %= L
    return pltpu.roll(a, shift, 1) if shift else a


def ring_east(tiles, lane):
    turned = [turn(a, -1) for a in tiles]
    if len(tiles) == 1:
        return turned
    return [jnp.where(lane < L - 1, a, turned[(i + 1) % len(tiles)]) for i, a in enumerate(turned)]


def ring_west(tiles, lane):
    turned = [turn(a, 1) for a in tiles]
    if len(tiles) == 1:
        return turned
    return [jnp.where(lane > 0, a, turned[i - 1]) for i, a in enumerate(turned)]


def rows(at):
    return pl.ds(at, 8)


def kernel(
    ngy, ngx,
    tr_hbm, ea_hbm, no_hbm, co_hbm, th_hbm, sf_hbm, he_hbm,
    tr_out, h_out,
    th, a, ci, cf, s, c1, c2, c1s, c2s, fl, fls, me_s, mn_s, mes_s, mns_s, fx, fs,
    pw, pe, re, rw, v0_s, v1_s, v2_s, sh_s, inv_s, wet_s, row, b1, b2,
    load_sem, send_sem, recv_sem, rs_sem, rr_sem,
):
    f32 = jnp.float32
    gy, gx = lax.axis_index("gy"), lax.axis_index("gx")
    north, south = lax.rem(gy + 1, ngy), lax.rem(gy + ngy - 1, ngy)
    e_id, w_id = lax.rem(gx + 1, ngx), lax.rem(gx + ngx - 1, ngx)
    hi, z = lax.div(gx, 8), lax.rem(gx, 8)
    group1 = [
        (lax.rem(gy + dy, ngy), lax.rem(gx + 8 * dh, ngx))
        for dh in range(2) for dy in range(16) if dy or dh
    ]
    far1 = [device for i, device in enumerate(group1) if i not in (0, 14)]
    group2 = [(gy, hi * 8 + lax.rem(z + dz, 8)) for dz in range(1, 8)]
    near = [(north, gx), (south, gx), (gy, e_id), (gy, w_id),
            (north, e_id), (north, w_id), (south, e_id), (south, w_id)]

    barrier = pltpu.get_barrier_semaphore()

    def greet(devices):
        for y, x in devices:
            pl.semaphore_signal(barrier, inc=1, device_id={"gy": y, "gx": x}, device_id_type=MESH)

    greet(near)
    own, both = pl.ds(8, R), pl.ds(0, 2)
    halves = [pl.ds(0, L), pl.ds(L, L)]
    for g in range(K // PAIR):
        for src, base in ((tr_hbm, TR), (ea_hbm, EA), (no_hbm, NO)):
            for i, half in enumerate(halves):
                pltpu.make_async_copy(
                    src.at[pl.ds(PAIR * g, PAIR), :, half], a.at[pl.ds(base + PAIR * g, PAIR), i, own], load_sem.at[g]
                ).start()
    for src, dst in ((sf_hbm, a.at[SF]), (he_hbm, a.at[HE]), (co_hbm, ci)):
        for i, half in enumerate(halves):
            pltpu.make_async_copy(src.at[:, half], dst.at[i, own], load_sem.at[K // PAIR]).start()
    th_load = pltpu.make_async_copy(th_hbm, th, load_sem.at[K // PAIR + 1])
    th_load.start()
    greet(far1 + group2)

    def wait_rows(ref, sem):
        pltpu.make_async_copy(ref, ref, sem).wait()

    lane = lax.broadcasted_iota(jnp.int32, (8, L), 1)
    tiles = range(R // 8)

    packs = [[jnp.zeros((8, L), f32) for _ in tiles] for _ in range(2)]
    for g in range(K // PAIR + 1):
        wait_rows(a.at[pl.ds(0, 3 * PAIR if g < K // PAIR else 3), both, own], load_sem.at[g])
        for field, at, first, last in PLAN[3 * PAIR * g : 3 * PAIR * (g + 1)]:
            for side in range(2):
                width = last if side else first
                start = at - 8 - width if side else at
                mask = window(lane, start, width)
                shift = at - 8 if side else at
                for t in tiles:
                    if field == CO:
                        value = ci[side, rows(8 + 8 * t), :].astype(f32)
                    else:
                        value = a[field, side, rows(8 + 8 * t), :]
                    packs[side][t] = jnp.where(mask, turn(value, shift), packs[side][t])
    for side, dest in enumerate((pw, pe)):
        for t in tiles:
            dest[rows(8 * t), :] = packs[side][t]

    pl.semaphore_wait(barrier, len(near) + len(far1) + len(group2))

    top, bottom = pl.ds(R + 3, HALO), pl.ds(8, HALO)
    ghost_s, ghost_n = pl.ds(3, HALO), pl.ds(R + 8, HALO)
    every = pl.ds(0, NF)

    def send(kind, src, dst, y, x):
        pltpu.make_async_remote_copy(
            src_ref=src, dst_ref=dst, send_sem=send_sem.at[kind], recv_sem=recv_sem.at[kind],
            device_id={"gy": y, "gx": x}, device_id_type=MESH,
        ).start()

    has_north, has_south = gy < ngy - 1, gy > 0

    @pl.when(has_north)
    def _():
        send(1, pe.at[pl.ds(R - HALO, HALO)], rw.at[ghost_s], north, e_id)
        send(1, pw.at[pl.ds(R - HALO, HALO)], re.at[ghost_s], north, w_id)

    @pl.when(has_south)
    def _():
        send(2, pe.at[pl.ds(0, HALO)], rw.at[ghost_n], south, e_id)
        send(2, pw.at[pl.ds(0, HALO)], re.at[ghost_n], south, w_id)

    send(0, pe, rw.at[own], gy, e_id)
    send(0, pw, re.at[own], gy, w_id)

    @pl.when(has_north)
    def _():
        send(1, ci.at[both, top], ci.at[both, ghost_s], north, gx)
        send(1, a.at[every, both, top], a.at[every, both, ghost_s], north, gx)

    @pl.when(has_south)
    def _():
        send(2, ci.at[both, bottom], ci.at[both, ghost_n], south, gx)
        send(2, a.at[every, both, bottom], a.at[every, both, ghost_n], south, gx)

    column_rows = (1, 2, R)
    row_rows = (1, 2, HALO * (NF + 2))
    assert RE >= HALO * (NF + 2)

    def sized(shape):
        return c1.at[pl.ds(0, shape[0]), pl.ds(0, shape[1]), pl.ds(0, shape[2])]

    def each_end(sem):
        @pl.when(has_north if sem is send_sem else has_south)
        def _():
            wait_rows(sized(row_rows), sem.at[1])

        @pl.when(has_south if sem is send_sem else has_north)
        def _():
            wait_rows(sized(row_rows), sem.at[2])

    zero8 = jnp.zeros((8, L), f32)
    for at0, open_end in ((0, has_south), (R + 8, has_north)):

        @pl.when(jnp.logical_not(open_end))
        def _(at0=at0):
            for i in range(2):
                ci[i, rows(at0), :] = jnp.zeros((8, L), jnp.int32)
                for field in range(NF):
                    a[field, i, rows(at0), :] = zero8
            re[rows(at0), :] = zero8
            rw[rows(at0), :] = zero8

    th_load.wait()

    def seam(field, at):
        left, right = (cf[0, rows(at), :], cf[1, rows(at), :]) if field == CO else (
            a[field, 0, rows(at), :], a[field, 1, rows(at), :])
        return jnp.where(lane < 64, turn(right, 4), turn(left, -4))

    def diagonal(i, at, helm, depth):
        inv_s[i, rows(at), :] = 1.0 / (6.0 + helm)
        wet_s[i, rows(at), :] = jnp.where(depth > 0.0, 1.0, 0.0)

    for i in range(2):
        for t in tiles:
            at = 8 + 8 * t
            cf[i, rows(at), :] = ci[i, rows(at), :].astype(f32)
            fx[i, rows(at), :] = a[SF, i, rows(at), :]
            diagonal(i, at, a[HE, i, rows(at), :], cf[i, rows(at), :])
    for field in range(NF + 1):
        for t in tiles:
            s[field, rows(8 + 8 * t), :] = seam(field, 8 + 8 * t)

    def face_masks(at, below):
        depth = [cf[i, rows(at), :] for i in range(2)]
        for i, other in enumerate(ring_east(depth, lane)):
            me_s[i, rows(at), :] = jnp.minimum(depth[i], other)
            mn_s[i, rows(below), :] = jnp.minimum(cf[i, rows(below), :], cf[i, rows(below + 1), :])

    for t in tiles:
        face_masks(8 + 8 * t, min(8 + 8 * t, R - 1))

    def north_flux(k, kf, i, current, at):
        speed = jnp.where(mn_s[i, rows(at), :] > kf, a[NO + k, i, rows(at), :], 0.0)
        return speed * jnp.where(speed > 0.0, current(i, at), current(i, at + 1))

    def east_flux(k, kf, now, at):
        out = []
        for i, other in enumerate(ring_east(now, lane)):
            speed = jnp.where(me_s[i, rows(at), :] > kf, a[EA + k, i, rows(at), :], 0.0)
            out.append(speed * jnp.where(speed > 0.0, now[i], other))
        return out

    def own_step(k, kf, current, store, starts, direct):
        if not direct:
            for at in [at - 1 for at in starts] + [starts[-1]]:
                for i in range(2):
                    fl[i, rows(at), :] = north_flux(k, kf, i, current, at)
        for at in starts:
            now = [current(i, at) for i in range(2)]
            fe = east_flux(k, kf, now, at)
            fw = ring_west(fe, lane)
            for i in range(2):
                if direct:
                    fn, fb = north_flux(k, kf, i, current, at), north_flux(k, kf, i, current, at - 1)
                else:
                    fn, fb = fl[i, rows(at), :], fl[i, rows(at - 1), :]
                store(i, at, now[i] - (fe[i] - fw[i] + fn - fb))

    def own_levels(k, starts1, starts2, direct):
        kf = k.astype(f32)
        weight = th[k]

        def put1(i, at, value):
            c1[k, i, rows(at), :] = value

        def put2(i, at, value):
            c2[k, i, rows(at), :] = value
            fx[i, rows(at), :] += jnp.where(cf[i, rows(at), :] > kf, weight * value, 0.0)

        own_step(k, kf, lambda i, at: a[TR + k, i, rows(at), :], put1, starts1, direct)
        own_step(k, kf, lambda i, at: c1[k, i, rows(at), :], put2, starts2, direct)

    starts1 = [9 + 8 * t for t in range(15)] + [R - 1]
    starts2 = [12 + 8 * t for t in range(15)]

    def interior(k, carry):
        own_levels(k, starts1, starts2, False)
        return carry

    lax.fori_loop(0, K, interior, 0)

    wait_rows(sized(column_rows), recv_sem.at[0])

    ghosts = window(lane, 4, HALO) | window(lane, 119, HALO)
    ends = (0, R + 8)

    def unpack(spots, beneath):
        from_east = [re[rows(at), :] for at in spots]
        from_west = [rw[rows(at), :] for at in spots]
        for field, at, first, _ in PLAN:
            mask = window(lane, at, first)
            for j, spot in enumerate(spots):
                value = turn(jnp.where(mask, from_east[j], from_west[j]), 4 - at)
                s[field, rows(spot), :] = jnp.where(ghosts, value, beneath(field, spot))

    for first_row in (8, 72):
        unpack([first_row + 8 * t for t in range(8)], lambda field, at: s[field, rows(at), :])

    def beside(tile):
        return turn(tile, 4), turn(tile, -4)

    def ghost_tile(field, at):
        west, east = beside(s[field, rows(at), :])
        return jnp.where(lane < 64, east, west)

    for t in tiles:
        at = 8 + 8 * t
        depth = s[CO, rows(at), :]
        mes_s[rows(at), :] = jnp.minimum(depth, turn(depth, -1))
        below = min(at, R - 1)
        mns_s[rows(below), :] = jnp.minimum(s[CO, rows(below), :], s[CO, rows(below + 1), :])
        fs[rows(at), :] = s[SF, rows(at), :]
        diagonal(2, at, ghost_tile(HE, at), ghost_tile(CO, at))

    def seam_flux(k, kf, current, at):
        speed = jnp.where(mns_s[rows(at), :] > kf, s[NO + k, rows(at), :], 0.0)
        return speed * jnp.where(speed > 0.0, current(at), current(at + 1))

    def seam_step(k, j, kf, current, store, starts, direct):
        if not direct:
            for at in [at - 1 for at in starts] + [starts[-1]]:
                fls[j, rows(at), :] = seam_flux(k, kf, current, at)
        for at in starts:
            now = current(at)
            speed = jnp.where(mes_s[rows(at), :] > kf, s[EA + k, rows(at), :], 0.0)
            fe = speed * jnp.where(speed > 0.0, now, turn(now, -1))
            if direct:
                fn, fb = seam_flux(k, kf, current, at), seam_flux(k, kf, current, at - 1)
            else:
                fn, fb = fls[j, rows(at), :], fls[j, rows(at - 1), :]
            store(at, now - (fe - turn(fe, 1) + fn - fb))

    def seam_levels(k, j, starts1, starts2, direct):
        kf = k.astype(f32)
        weight = th[k]

        def put1(at, value):
            c1s[k, rows(at), :] = value

        def put2(at, value):
            c2s[k, rows(at), :] = value
            fs[rows(at), :] += jnp.where(s[CO, rows(at), :] > kf, weight * value, 0.0)

        seam_step(k, j, kf, lambda at: s[TR + k, rows(at), :], put1, starts1, direct)
        seam_step(k, j, kf, lambda at: c1s[k, rows(at), :], put2, starts2, direct)

    def seams(step, carry):
        for j in range(UNROLL):
            seam_levels(step * UNROLL + j, j, starts1, starts2, False)
        return carry

    lax.fori_loop(0, K // UNROLL, seams, 0)

    each_end(recv_sem)

    for at in ends:
        for i in range(2):
            cf[i, rows(at), :] = ci[i, rows(at), :].astype(f32)
    unpack(ends, seam)

    strips = (4, R + 4)
    for at in strips:
        face_masks(at, at - 1)
        below = at + 1
        for i in range(2):
            mn_s[i, rows(below), :] = jnp.minimum(cf[i, rows(below), :], cf[i, rows(below + 1), :])
            fx[i, rows(at), :] = a[SF, i, rows(at), :]
        depth = s[CO, rows(at), :]
        mes_s[rows(at), :] = jnp.minimum(depth, turn(depth, -1))
        for below in (at - 1, at + 1):
            mns_s[rows(below), :] = jnp.minimum(s[CO, rows(below), :], s[CO, rows(below + 1), :])
        fs[rows(at), :] = s[SF, rows(at), :]
    for at in ends:
        for i in range(2):
            diagonal(i, at, a[HE, i, rows(at), :], cf[i, rows(at), :])
        diagonal(2, at, ghost_tile(HE, at), ghost_tile(CO, at))

    def edges(step, carry):
        for j in range(STRIP_UNROLL):
            k = step * STRIP_UNROLL + j
            own_levels(k, strips, strips, True)
            seam_levels(k, j, strips, strips, True)
        return carry

    lax.fori_loop(0, K // STRIP_UNROLL, edges, 0)

    blocks = [1] + [8 * t for t in range(1, 18)]
    inside = [8 * t for t in range(1, 17)]

    for at in blocks:
        f_w, f_e = beside(fs[rows(at), :])
        forcing = [
            jnp.where(lane < 2, f_w, fx[0, rows(at), :]),
            jnp.where(lane >= L - 2, f_e, fx[1, rows(at), :]),
            jnp.where(lane < 64, f_e, f_w),
        ]
        for i in range(3):
            fx[i, rows(at), :] = forcing[i]
            v0_s[i, rows(at), :] = forcing[i] * inv_s[i, rows(at), :]

    nu = [[jnp.zeros((8, L), f32) for _ in range(2)] for _ in range(6)]

    def operator(n, src, spots, store):
        spread = {}
        for at in blocks:
            w = [src[i, rows(at), :] for i in range(3)]
            if n == 0:
                w = [wet_s[i, rows(at), :] * w[i] for i in range(3)]
            h = [x + y for x, y in zip(ring_west(w, lane), ring_east(w, lane))]
            spread[at] = h
            for i in range(3):
                sh_s[n, i, rows(at), :] = w[i] + 0.5 * h[i]
        for at in spots:
            for i in range(3):
                u = wet_s[i, rows(at), :] * (
                    spread[at][i] + sh_s[n, i, rows(at + 1), :] + sh_s[n, i, rows(at - 1), :])
                store(i, at, u)

    def counted(i, at):
        return i < 2 and at in inside

    def store1(i, at, u):
        v = u * inv_s[i, rows(at), :]
        v1_s[i, rows(at), :] = v
        if counted(i, at):
            f = fx[i, rows(at), :]
            nu[0][i] += f * v0_s[i, rows(at), :]
            nu[1][i] += v * f
            nu[2][i] += v * u

    def store2(i, at, u):
        v = u * inv_s[i, rows(at), :]
        v2_s[i, rows(at), :] = v
        if counted(i, at):
            nu[3][i] += v1_s[i, rows(at), :] * u
            nu[4][i] += v * u

    def store3(i, at, u):
        if counted(i, at):
            nu[5][i] += v2_s[i, rows(at), :] * u

    operator(0, v0_s, blocks, store1)
    operator(1, v1_s, blocks, store2)
    operator(2, v2_s, inside, store3)

    def finish_tracer():
        def put(k, carry):
            for t in tiles:
                at = 8 + 8 * t
                turned = beside(c2s[k, rows(at), :])
                for i, mask in enumerate((lane < 2, lane >= L - 2)):
                    tr_out[k, rows(8 * t), halves[i]] = jnp.where(mask, turned[i], c2[k, i, rows(at), :])
            return carry

        lax.fori_loop(0, K, put, 0)

    lane1 = lax.broadcasted_iota(jnp.int32, (1, 128), 1)
    packed = jnp.zeros((1, 128), jnp.float32)
    for i, part in enumerate(nu):
        lanes = jnp.sum(part[0] + part[1], axis=0, keepdims=True)
        total = jnp.sum(lanes, axis=1, keepdims=True)
        packed = jnp.where(lane1 == i, total, packed)

    reduce_sends = []
    for i, (group, slot, buf) in enumerate(((group1, gy * 2 + hi, b1), (group2, z, b2))):
        row[i] = packed
        n = len(group)
        for y, x in group:
            copy = pltpu.make_async_remote_copy(
                src_ref=row.at[i], dst_ref=buf.at[slot], send_sem=rs_sem.at[i], recv_sem=rr_sem.at[i],
                device_id={"gy": y, "gx": x}, device_id_type=MESH,
            )
            copy.start()
        buf[slot] = packed
        if i == 0:
            finish_tracer()
        pltpu.make_async_copy(buf.at[pl.ds(0, n)], buf.at[pl.ds(0, n)], rr_sem.at[i]).wait()
        reduce_sends.append((buf, n, i))
        packed = jnp.sum(buf[...], axis=0)

    m = [jnp.sum(jnp.where(lane1 == i, packed, 0.0), axis=1, keepdims=True) for i in range(6)]

    def form(p, moments):
        total = None
        for i, pi in enumerate(p):
            for j, pj in enumerate(p[i:], i):
                term = (pi * pj if i == j else 2.0 * pi * pj) * moments[i + j]
                total = term if total is None else total + term
        return total

    diff = [m[i] - m[i + 1] for i in range(5)]
    one = jnp.ones_like(m[0])
    zc, pc = [one], [one]
    heights = [jnp.zeros_like(one)] * 3
    rz = m[0]
    for it in range(ITERS):
        alpha = rz / form(pc, diff)
        heights = [h + alpha * pc[i] if i < len(pc) else h for i, h in enumerate(heights)]
        if it + 1 < ITERS:
            applied = [p - q for p, q in zip(pc + [jnp.zeros_like(one)], [jnp.zeros_like(one)] + pc)]
            zc = [(zc[i] if i < len(zc) else 0.0) - alpha * applied[i] for i in range(len(applied))]
            rz_next = form(zc, m)
            beta = rz_next / rz
            pc = [zc[i] + beta * pc[i] if i < len(pc) else zc[i] for i in range(len(zc))]
            rz = rz_next

    for t in tiles:
        at = 8 + 8 * t
        for i in range(2):
            h_out[rows(8 * t), halves[i]] = (
                heights[0] * v0_s[i, rows(at), :] + heights[1] * v1_s[i, rows(at), :] + heights[2] * v2_s[i, rows(at), :])

    wait_rows(sized(column_rows), send_sem.at[0])
    each_end(send_sem)
    for buf, n, i in reduce_sends:
        pltpu.make_async_copy(buf.at[pl.ds(0, n)], buf.at[pl.ds(0, n)], rs_sem.at[i]).wait()


def put_kernel(tr, h, tr_hbm, h_hbm, sem):
    copies = [pltpu.make_async_copy(tr, tr_hbm, sem.at[0]), pltpu.make_async_copy(h, h_hbm, sem.at[1])]
    for copy in copies:
        copy.start()
    for copy in copies:
        copy.wait()


def on_device(ngy, ngx, tracer, east_speed, north_speed, columns, thickness, surface_flux, helm):
    f32 = jnp.float32
    any_spec = pl.BlockSpec(memory_space=pltpu.HBM)
    vmem = pl.BlockSpec(memory_space=pltpu.VMEM)
    results = pl.pallas_call(
        functools.partial(kernel, ngy, ngx),
        out_shape=(pltpu.VMEM((K, R, C), f32), pltpu.VMEM((R, C), f32)),
        in_specs=[any_spec, any_spec, any_spec, any_spec, any_spec, any_spec, any_spec],
        out_specs=(vmem, vmem),
        scratch_shapes=[
            pltpu.SMEM((K,), f32),
            pltpu.VMEM((NF, 2, RE, L), f32),
            pltpu.VMEM((2, RE, L), jnp.int32),
            pltpu.VMEM((2, RE, L), f32),
            pltpu.VMEM((NF + 1, RE, L), f32),
            pltpu.VMEM((K, 2, RE, L), f32),
            pltpu.VMEM((K, 2, RE, L), f32),
            pltpu.VMEM((K, RE, L), f32),
            pltpu.VMEM((K, RE, L), f32),
            pltpu.VMEM((2, RE, L), f32),
            pltpu.VMEM((UNROLL, RE, L), f32),
            pltpu.VMEM((2, RE, L), f32),
            pltpu.VMEM((2, RE, L), f32),
            pltpu.VMEM((RE, L), f32),
            pltpu.VMEM((RE, L), f32),
            pltpu.VMEM((3, RE, L), f32),
            pltpu.VMEM((RE, L), f32),
            pltpu.VMEM((R, L), f32),
            pltpu.VMEM((R, L), f32),
            pltpu.VMEM((RE, L), f32),
            pltpu.VMEM((RE, L), f32),
            pltpu.VMEM((3, RE, L), f32),
            pltpu.VMEM((3, RE, L), f32),
            pltpu.VMEM((3, RE, L), f32),
            pltpu.VMEM((3, 3, RE, L), f32),
            pltpu.VMEM((3, RE, L), f32),
            pltpu.VMEM((3, RE, L), f32),
            pltpu.VMEM((2, 1, L), f32),
            pltpu.VMEM((32, 1, L), f32),
            pltpu.VMEM((8, 1, L), f32),
            pltpu.SemaphoreType.DMA((K // PAIR + 2,)),
            pltpu.SemaphoreType.DMA((3,)),
            pltpu.SemaphoreType.DMA((3,)),
            pltpu.SemaphoreType.DMA((2,)),
            pltpu.SemaphoreType.DMA((2,)),
        ],
        compiler_params=pltpu.CompilerParams(collective_id=0, has_side_effects=True),
    )(tracer, east_speed, north_speed, columns, thickness, surface_flux, helm)
    return pl.pallas_call(
        put_kernel,
        out_shape=(jax.ShapeDtypeStruct((K, R, C), f32), jax.ShapeDtypeStruct((R, C), f32)),
        in_specs=[vmem, vmem],
        out_specs=(any_spec, any_spec),
        scratch_shapes=[pltpu.SemaphoreType.DMA((2,))],
    )(*[pltpu.with_memory_space_constraint(r, pltpu.VMEM) for r in results])


def solution(mesh):
    sizes = mesh.shape
    cells, plane = P(None, "gy", "gx"), P("gy", "gx")
    return jax.shard_map(
        functools.partial(on_device, sizes["gy"], sizes["gx"]),
        mesh=mesh,
        in_specs=(cells, cells, cells, plane, P(), plane, plane),
        out_specs=(cells, plane),
        check_vma=False,
    )
```

```python
import functools

import jax
import jax.numpy as jnp
from jax import lax
from jax.experimental import pallas as pl
from jax.experimental.pallas import tpu as pltpu
from jax.sharding import PartitionSpec as P

ITERS = 3
K = 8
R, C, L = 128, 256, 128
RE = R + 24
HALO = 5
MESH = pl.DeviceIdType.MESH
TR, EA, NO, SF, HE, CO = 0, K, 2 * K, 3 * K, 3 * K + 1, 3 * K + 2
NF = 3 * K + 2
STRIP_UNROLL = 8
PAIR = 2


SLOT = 32
QUADS = 4
STARTS = {TR: (0, 14), EA: (5, 19), NO: (9, 23)}
WIDTHS = {TR: (5, 5), EA: (4, 5), NO: (4, 4)}
PLANES = ((CO, 27, 4), (SF, 59, 3), (HE, 91, 3))
S_SF, S_HE, S_CO = 6, 7, 8


def lane_plan():
    plan = [(field, at, width, width) for field, at, width in PLANES]
    for k in range(K):
        for base in (TR, EA, NO):
            plan.append((base + k, SLOT * (k % QUADS) + STARTS[base][k // QUADS]) + WIDTHS[base])
    return plan


PLAN = lane_plan()


def window(lane, start, width):
    start %= L
    if start + width <= L:
        return (lane >= start) & (lane < start + width)
    return (lane >= start) | (lane < start + width - L)


def turn(a, shift):
    shift %= L
    return pltpu.roll(a, shift, 1) if shift else a


def ring_east(tiles, lane):
    turned = [turn(a, -1) for a in tiles]
    if len(tiles) == 1:
        return turned
    return [jnp.where(lane < L - 1, a, turned[(i + 1) % len(tiles)]) for i, a in enumerate(turned)]


def ring_west(tiles, lane):
    turned = [turn(a, 1) for a in tiles]
    if len(tiles) == 1:
        return turned
    return [jnp.where(lane > 0, a, turned[i - 1]) for i, a in enumerate(turned)]


def rows(at):
    return pl.ds(at, 8)


def kernel(
    ngy, ngx,
    tr_hbm, ea_hbm, no_hbm, co_hbm, th_hbm, sf_hbm, he_hbm,
    tr_out, h_out,
    th, a, ci, cf, s, c1, c2, c1s, c2s, fl, fls, me_s, mn_s, mes_s, mns_s, fx, fs,
    pw, pe, re, rw, v0_s, v1_s, v2_s, sh_s, inv_s, wet_s, row, b1, b2,
    load_sem, send_sem, recv_sem, rs_sem, rr_sem,
):
    f32 = jnp.float32
    gy, gx = lax.axis_index("gy"), lax.axis_index("gx")
    north, south = lax.rem(gy + 1, ngy), lax.rem(gy + ngy - 1, ngy)
    e_id, w_id = lax.rem(gx + 1, ngx), lax.rem(gx + ngx - 1, ngx)
    hi, z = lax.div(gx, 8), lax.rem(gx, 8)
    group1 = [
        (lax.rem(gy + dy, ngy), lax.rem(gx + 8 * dh, ngx))
        for dh in range(2) for dy in range(16) if dy or dh
    ]
    far1 = [device for i, device in enumerate(group1) if i not in (0, 14)]
    group2 = [(gy, hi * 8 + lax.rem(z + dz, 8)) for dz in range(1, 8)]
    near = [(north, gx), (south, gx), (gy, e_id), (gy, w_id),
            (north, e_id), (north, w_id), (south, e_id), (south, w_id)]

    barrier = pltpu.get_barrier_semaphore()

    def greet(devices):
        for y, x in devices:
            pl.semaphore_signal(barrier, inc=1, device_id={"gy": y, "gx": x}, device_id_type=MESH)

    greet(near)
    own, both = pl.ds(8, R), pl.ds(0, 2)
    halves = [pl.ds(0, L), pl.ds(L, L)]
    for src, dst in ((sf_hbm, a.at[SF]), (he_hbm, a.at[HE]), (co_hbm, ci)):
        for i, half in enumerate(halves):
            pltpu.make_async_copy(src.at[:, half], dst.at[i, own], load_sem.at[K // PAIR]).start()
    for g in range(K // PAIR):
        for src, base in ((tr_hbm, TR), (ea_hbm, EA), (no_hbm, NO)):
            for i, half in enumerate(halves):
                pltpu.make_async_copy(
                    src.at[pl.ds(PAIR * g, PAIR), :, half], a.at[pl.ds(base + PAIR * g, PAIR), i, own], load_sem.at[g]
                ).start()
    th_load = pltpu.make_async_copy(th_hbm, th, load_sem.at[K // PAIR + 1])
    th_load.start()
    greet(far1 + group2)

    def wait_rows(ref, sem):
        pltpu.make_async_copy(ref, ref, sem).wait()

    lane = lax.broadcasted_iota(jnp.int32, (8, L), 1)
    tiles = range(R // 8)

    packs = [[jnp.zeros((8, L), f32) for _ in tiles] for _ in range(2)]
    for g in range(-1, K // PAIR):
        wait_rows(a.at[pl.ds(0, 3 if g < 0 else 3 * PAIR), both, own], load_sem.at[g if g >= 0 else K // PAIR])
        if g < 0:
            for side in range(2):
                for t in tiles:
                    depth = ci[side, rows(8 + 8 * t), :].astype(f32)
                    beyond = turn(depth, -1)
                    if side:
                        beyond = jnp.where(lane == L - 1, float(K), beyond)
                    sh_s[0, side, rows(8 * t), :] = jnp.minimum(depth, beyond)
        begin = 0 if g < 0 else 3 + 3 * PAIR * g
        for field, at, first, last in PLAN[begin : begin + (3 if g < 0 else 3 * PAIR)]:
            for side in range(2):
                width = last if side else first
                mask = window(lane, at - 8 - width if side else at, width)
                shift = at - 8 if side else at
                for t in tiles:
                    if field == CO:
                        value = ci[side, rows(8 + 8 * t), :].astype(f32)
                    else:
                        value = a[field, side, rows(8 + 8 * t), :]
                    if EA <= field < NO:
                        value = jnp.where(sh_s[0, side, rows(8 * t), :] > float(field - EA), value, 0.0)
                    packs[side][t] = jnp.where(mask, turn(value, shift), packs[side][t])
    for side, dest in enumerate((pw, pe)):
        for t in tiles:
            dest[rows(8 * t), :] = packs[side][t]

    pl.semaphore_wait(barrier, len(near) + len(far1) + len(group2))

    top, bottom = pl.ds(R + 3, HALO), pl.ds(8, HALO)
    ghost_s, ghost_n = pl.ds(3, HALO), pl.ds(R + 8, HALO)
    every = pl.ds(0, NF)

    def send(kind, src, dst, y, x):
        pltpu.make_async_remote_copy(
            src_ref=src, dst_ref=dst, send_sem=send_sem.at[kind], recv_sem=recv_sem.at[kind],
            device_id={"gy": y, "gx": x}, device_id_type=MESH,
        ).start()

    has_north, has_south = gy < ngy - 1, gy > 0

    @pl.when(has_north)
    def _():
        send(1, pe.at[pl.ds(R - HALO, HALO)], rw.at[ghost_s], north, e_id)
        send(1, pw.at[pl.ds(R - HALO, HALO)], re.at[ghost_s], north, w_id)

    @pl.when(has_south)
    def _():
        send(2, pe.at[pl.ds(0, HALO)], rw.at[ghost_n], south, e_id)
        send(2, pw.at[pl.ds(0, HALO)], re.at[ghost_n], south, w_id)

    send(0, pe, rw.at[own], gy, e_id)
    send(0, pw, re.at[own], gy, w_id)

    @pl.when(has_north)
    def _():
        send(1, ci.at[both, top], ci.at[both, ghost_s], north, gx)
        send(1, a.at[every, both, top], a.at[every, both, ghost_s], north, gx)

    @pl.when(has_south)
    def _():
        send(2, ci.at[both, bottom], ci.at[both, ghost_n], south, gx)
        send(2, a.at[every, both, bottom], a.at[every, both, ghost_n], south, gx)

    column_rows = (1, 2, R)
    row_rows = (1, 2, HALO * (NF + 2))
    assert RE >= HALO * (NF + 2)

    def sized(shape):
        return c1.at[pl.ds(0, shape[0]), pl.ds(0, shape[1]), pl.ds(0, shape[2])]

    def each_end(sem):
        @pl.when(has_north if sem is send_sem else has_south)
        def _():
            wait_rows(sized(row_rows), sem.at[1])

        @pl.when(has_south if sem is send_sem else has_north)
        def _():
            wait_rows(sized(row_rows), sem.at[2])

    zero8 = jnp.zeros((8, L), f32)
    for at0, open_end in ((0, has_south), (R + 8, has_north)):

        @pl.when(jnp.logical_not(open_end))
        def _(at0=at0):
            for i in range(2):
                ci[i, rows(at0), :] = jnp.zeros((8, L), jnp.int32)
                for field in range(NF):
                    a[field, i, rows(at0), :] = zero8
            re[rows(at0), :] = zero8
            rw[rows(at0), :] = zero8

    th_load.wait()

    def seam(field, at):
        left, right = (cf[0, rows(at), :], cf[1, rows(at), :]) if field == CO else (
            a[field, 0, rows(at), :], a[field, 1, rows(at), :])
        return jnp.where(lane < 64, turn(right, 4), turn(left, -4))

    def seam_quad(base, half, at):
        tile = jnp.zeros((8, L), f32)
        for q in range(QUADS):
            field = base + QUADS * half + q
            tile = jnp.where(window(lane, SLOT * q, 4), turn(a[field, 1, rows(at), :], SLOT * q + 4), tile)
            tile = jnp.where(window(lane, SLOT * q - 4, 4), turn(a[field, 0, rows(at), :], SLOT * q - 4), tile)
        return tile

    quads = [(base, half) for base in (TR, EA, NO) for half in range(2)]
    planes = ((S_SF, SF), (S_HE, HE), (S_CO, CO))

    def own_seam(tile, at):
        return seam_quad(*quads[tile], at) if tile < 6 else seam(planes[tile - 6][1], at)

    def diagonal(i, at, helm, depth):
        inv_s[i, rows(at), :] = 1.0 / (6.0 + helm)
        wet_s[i, rows(at), :] = jnp.where(depth > 0.0, 1.0, 0.0)

    for i in range(2):
        for t in tiles:
            at = 8 + 8 * t
            cf[i, rows(at), :] = ci[i, rows(at), :].astype(f32)
            fx[i, rows(at), :] = a[SF, i, rows(at), :]
            diagonal(i, at, a[HE, i, rows(at), :], cf[i, rows(at), :])
    for tile in range(9):
        for t in tiles:
            s[tile, rows(8 + 8 * t), :] = own_seam(tile, 8 + 8 * t)

    def face_masks(at, below):
        depth = [cf[i, rows(at), :] for i in range(2)]
        for i, other in enumerate(ring_east(depth, lane)):
            me_s[i, rows(at), :] = jnp.minimum(depth[i], other)
            mn_s[i, rows(below), :] = jnp.minimum(cf[i, rows(below), :], cf[i, rows(below + 1), :])

    for t in tiles:
        face_masks(8 + 8 * t, min(8 + 8 * t, R - 1))

    def north_flux(k, kf, i, current, at):
        speed = jnp.where(mn_s[i, rows(at), :] > kf, a[NO + k, i, rows(at), :], 0.0)
        return speed * jnp.where(speed > 0.0, current(i, at), current(i, at + 1))

    def east_flux(k, kf, now, at):
        out = []
        for i, other in enumerate(ring_east(now, lane)):
            speed = jnp.where(me_s[i, rows(at), :] > kf, a[EA + k, i, rows(at), :], 0.0)
            out.append(speed * jnp.where(speed > 0.0, now[i], other))
        return out

    def own_step(k, kf, current, store, starts, direct):
        if not direct:
            for at in [at - 1 for at in starts] + [starts[-1]]:
                for i in range(2):
                    fl[i, rows(at), :] = north_flux(k, kf, i, current, at)
        for at in starts:
            now = [current(i, at) for i in range(2)]
            fe = east_flux(k, kf, now, at)
            fw = ring_west(fe, lane)
            for i in range(2):
                if direct:
                    fn, fb = north_flux(k, kf, i, current, at), north_flux(k, kf, i, current, at - 1)
                else:
                    fn, fb = fl[i, rows(at), :], fl[i, rows(at - 1), :]
                store(i, at, now[i] - (fe[i] - fw[i] + fn - fb))

    def own_levels(k, starts1, starts2, direct):
        kf = k.astype(f32)
        weight = th[k]

        def put1(i, at, value):
            c1[k, i, rows(at), :] = value

        def put2(i, at, value):
            c2[k, i, rows(at), :] = value
            fx[i, rows(at), :] += jnp.where(cf[i, rows(at), :] > kf, weight * value, 0.0)

        own_step(k, kf, lambda i, at: a[TR + k, i, rows(at), :], put1, starts1, direct)
        own_step(k, kf, lambda i, at: c1[k, i, rows(at), :], put2, starts2, direct)

    starts1 = [9 + 8 * t for t in range(15)] + [R - 1]
    starts2 = [12 + 8 * t for t in range(15)]

    def interior(k, carry):
        own_levels(k, starts1, starts2, False)
        return carry

    lax.fori_loop(0, K, interior, 0)

    wait_rows(sized(column_rows), recv_sem.at[0])

    within = lane & (SLOT - 1)
    ghosts = ((within >= 4) & (within < 9)) | ((within >= 23) & (within < 28))
    near_ghosts = window(lane, 4, 4) | window(lane, 120, 4)
    outer_ghosts = window(lane, 8, 1) | window(lane, 119, 1)
    own_lanes = window(lane, 124, 8)
    ends = (0, R + 8)

    def unpack(spots, beneath):
        from_east = [re[rows(at), :] for at in spots]
        from_west = [rw[rows(at), :] for at in spots]
        for tile in range(9):
            if tile < 6:
                base, half = quads[tile]
                start = STARTS[base][half]
                mask = ((lane - start) & (SLOT - 1)) < WIDTHS[base][0]
            else:
                start, width = {SF: (59, 3), HE: (91, 3), CO: (27, 4)}[planes[tile - 6][1]]
                mask = window(lane, start, width)
            for j, spot in enumerate(spots):
                value = turn(jnp.where(mask, from_east[j], from_west[j]), 4 - start)
                below = beneath(tile, spot)
                if tile == S_CO:
                    value = jnp.where(near_ghosts, value, jnp.where(own_lanes, below, 0.0))
                    value = jnp.where(outer_ghosts, float(K), value)
                    value = value + turn(value, SLOT)
                    value = value + turn(value, 2 * SLOT)
                else:
                    value = jnp.where(ghosts, value, below)
                s[tile, rows(spot), :] = value

    for first_row in (8, 72):
        unpack([first_row + 8 * t for t in range(8)], lambda tile, at: s[tile, rows(at), :])

    def beside(tile):
        return turn(tile, 4), turn(tile, -4)

    def ghost_tile(field, at):
        west, east = beside(s[field, rows(at), :])
        return jnp.where(lane < 64, east, west)

    for t in tiles:
        at = 8 + 8 * t
        depth = s[S_CO, rows(at), :]
        mes_s[rows(at), :] = jnp.minimum(depth, turn(depth, -1))
        below = min(at, R - 1)
        mns_s[rows(below), :] = jnp.minimum(s[S_CO, rows(below), :], s[S_CO, rows(below + 1), :])
        fs[rows(at), :] = zero8
        diagonal(2, at, ghost_tile(S_HE, at), ghost_tile(S_CO, at))

    slot = ((lane + SLOT // 2) // SLOT) & (QUADS - 1)
    floors = [(slot + QUADS * half).astype(f32) for half in range(2)]
    weights = []
    for half in range(2):
        weight = jnp.zeros((8, L), f32)
        for q in range(QUADS):
            weight = jnp.where(slot == q, th[QUADS * half + q], weight)
        weights.append(weight)

    def seam_flux(half, current, at):
        speed = jnp.where(mns_s[rows(at), :] > floors[half], s[4 + half, rows(at), :], 0.0)
        return speed * jnp.where(speed > 0.0, current(at), current(at + 1))

    def seam_step(half, current, store, starts, direct):
        if not direct:
            for at in [at - 1 for at in starts] + [starts[-1]]:
                fls[half, rows(at), :] = seam_flux(half, current, at)
        for at in starts:
            now = current(at)
            speed = jnp.where(mes_s[rows(at), :] > floors[half], s[2 + half, rows(at), :], 0.0)
            fe = speed * jnp.where(speed > 0.0, now, turn(now, -1))
            if direct:
                fn, fb = seam_flux(half, current, at), seam_flux(half, current, at - 1)
            else:
                fn, fb = fls[half, rows(at), :], fls[half, rows(at - 1), :]
            store(at, now - (fe - turn(fe, 1) + fn - fb))

    def seam_levels(half, starts1, starts2, direct):
        def put1(at, value):
            c1s[half, rows(at), :] = value

        def put2(at, value):
            c2s[half, rows(at), :] = value
            fs[rows(at), :] += jnp.where(s[S_CO, rows(at), :] > floors[half], weights[half] * value, 0.0)

        seam_step(half, lambda at: s[half, rows(at), :], put1, starts1, direct)
        seam_step(half, lambda at: c1s[half, rows(at), :], put2, starts2, direct)

    for half in range(2):
        seam_levels(half, starts1, starts2, False)

    each_end(recv_sem)

    for at in ends:
        for i in range(2):
            cf[i, rows(at), :] = ci[i, rows(at), :].astype(f32)
    unpack(ends, own_seam)

    strips = (4, R + 4)
    for at in strips:
        face_masks(at, at - 1)
        below = at + 1
        for i in range(2):
            mn_s[i, rows(below), :] = jnp.minimum(cf[i, rows(below), :], cf[i, rows(below + 1), :])
            fx[i, rows(at), :] = a[SF, i, rows(at), :]
        depth = s[S_CO, rows(at), :]
        mes_s[rows(at), :] = jnp.minimum(depth, turn(depth, -1))
        for below in (at - 1, at + 1):
            mns_s[rows(below), :] = jnp.minimum(s[S_CO, rows(below), :], s[S_CO, rows(below + 1), :])
        fs[rows(at), :] = zero8
    for at in ends:
        for i in range(2):
            diagonal(i, at, a[HE, i, rows(at), :], cf[i, rows(at), :])
        diagonal(2, at, ghost_tile(S_HE, at), ghost_tile(S_CO, at))

    def edges(step, carry):
        for j in range(STRIP_UNROLL):
            k = step * STRIP_UNROLL + j
            own_levels(k, strips, strips, True)
        return carry

    for half in range(2):
        seam_levels(half, strips, strips, True)
    lax.fori_loop(0, K // STRIP_UNROLL, edges, 0)

    blocks = [1] + [8 * t for t in range(1, 18)]
    inside = [8 * t for t in range(1, 17)]

    for at in blocks:
        folded = fs[rows(at), :]
        folded = folded + turn(folded, SLOT)
        f_w, f_e = beside(folded + turn(folded, 2 * SLOT) + s[S_SF, rows(at), :])
        forcing = [
            jnp.where(lane < 2, f_w, fx[0, rows(at), :]),
            jnp.where(lane >= L - 2, f_e, fx[1, rows(at), :]),
            jnp.where(lane < 64, f_e, f_w),
        ]
        for i in range(3):
            fx[i, rows(at), :] = forcing[i]
            v0_s[i, rows(at), :] = forcing[i] * inv_s[i, rows(at), :]

    nu = [[jnp.zeros((8, L), f32) for _ in range(2)] for _ in range(6)]

    def operator(n, src, spots, store):
        spread = {}
        for at in blocks:
            w = [src[i, rows(at), :] for i in range(3)]
            if n == 0:
                w = [wet_s[i, rows(at), :] * w[i] for i in range(3)]
            h = [x + y for x, y in zip(ring_west(w, lane), ring_east(w, lane))]
            spread[at] = h
            for i in range(3):
                sh_s[n, i, rows(at), :] = w[i] + 0.5 * h[i]
        for at in spots:
            for i in range(3):
                u = wet_s[i, rows(at), :] * (
                    spread[at][i] + sh_s[n, i, rows(at + 1), :] + sh_s[n, i, rows(at - 1), :])
                store(i, at, u)

    def counted(i, at):
        return i < 2 and at in inside

    def store1(i, at, u):
        v = u * inv_s[i, rows(at), :]
        v1_s[i, rows(at), :] = v
        if counted(i, at):
            f = fx[i, rows(at), :]
            nu[0][i] += f * v0_s[i, rows(at), :]
            nu[1][i] += v * f
            nu[2][i] += v * u

    def store2(i, at, u):
        v = u * inv_s[i, rows(at), :]
        v2_s[i, rows(at), :] = v
        if counted(i, at):
            nu[3][i] += v1_s[i, rows(at), :] * u
            nu[4][i] += v * u

    def store3(i, at, u):
        if counted(i, at):
            nu[5][i] += v2_s[i, rows(at), :] * u

    operator(0, v0_s, blocks, store1)
    operator(1, v1_s, blocks, store2)
    operator(2, v2_s, inside, store3)

    def finish_tracer():
        def put(half, carry):
            for q in range(QUADS):
                k = QUADS * half + q
                for t in tiles:
                    at = 8 + 8 * t
                    patch = c2s[half, rows(at), :]
                    patches = turn(patch, 4 - SLOT * q), turn(patch, -4 - SLOT * q)
                    for i, mask in enumerate((lane < 2, lane >= L - 2)):
                        tr_out[k, rows(8 * t), halves[i]] = jnp.where(mask, patches[i], c2[k, i, rows(at), :])
            return carry

        lax.fori_loop(0, K // QUADS, put, 0)

    lane1 = lax.broadcasted_iota(jnp.int32, (1, 128), 1)
    packed = jnp.zeros((1, 128), jnp.float32)
    for i, part in enumerate(nu):
        lanes = jnp.sum(part[0] + part[1], axis=0, keepdims=True)
        total = jnp.sum(lanes, axis=1, keepdims=True)
        packed = jnp.where(lane1 == i, total, packed)

    reduce_sends = []
    for i, (group, slot, buf) in enumerate(((group1, gy * 2 + hi, b1), (group2, z, b2))):
        row[i] = packed
        n = len(group)
        for y, x in group:
            copy = pltpu.make_async_remote_copy(
                src_ref=row.at[i], dst_ref=buf.at[slot], send_sem=rs_sem.at[i], recv_sem=rr_sem.at[i],
                device_id={"gy": y, "gx": x}, device_id_type=MESH,
            )
            copy.start()
        buf[slot] = packed
        if i == 0:
            finish_tracer()
        pltpu.make_async_copy(buf.at[pl.ds(0, n)], buf.at[pl.ds(0, n)], rr_sem.at[i]).wait()
        reduce_sends.append((buf, n, i))
        packed = jnp.sum(buf[...], axis=0)

    m = [jnp.sum(jnp.where(lane1 == i, packed, 0.0), axis=1, keepdims=True) for i in range(6)]

    def form(p, moments):
        total = None
        for i, pi in enumerate(p):
            for j, pj in enumerate(p[i:], i):
                term = (pi * pj if i == j else 2.0 * pi * pj) * moments[i + j]
                total = term if total is None else total + term
        return total

    diff = [m[i] - m[i + 1] for i in range(5)]
    one = jnp.ones_like(m[0])
    zc, pc = [one], [one]
    heights = [jnp.zeros_like(one)] * 3
    rz = m[0]
    for it in range(ITERS):
        alpha = rz / form(pc, diff)
        heights = [h + alpha * pc[i] if i < len(pc) else h for i, h in enumerate(heights)]
        if it + 1 < ITERS:
            applied = [p - q for p, q in zip(pc + [jnp.zeros_like(one)], [jnp.zeros_like(one)] + pc)]
            zc = [(zc[i] if i < len(zc) else 0.0) - alpha * applied[i] for i in range(len(applied))]
            rz_next = form(zc, m)
            beta = rz_next / rz
            pc = [zc[i] + beta * pc[i] if i < len(pc) else zc[i] for i in range(len(zc))]
            rz = rz_next

    for t in tiles:
        at = 8 + 8 * t
        for i in range(2):
            h_out[rows(8 * t), halves[i]] = (
                heights[0] * v0_s[i, rows(at), :] + heights[1] * v1_s[i, rows(at), :] + heights[2] * v2_s[i, rows(at), :])

    wait_rows(sized(column_rows), send_sem.at[0])
    each_end(send_sem)
    for buf, n, i in reduce_sends:
        pltpu.make_async_copy(buf.at[pl.ds(0, n)], buf.at[pl.ds(0, n)], rs_sem.at[i]).wait()


def put_kernel(tr, h, tr_hbm, h_hbm, sem):
    copies = [pltpu.make_async_copy(tr, tr_hbm, sem.at[0]), pltpu.make_async_copy(h, h_hbm, sem.at[1])]
    for copy in copies:
        copy.start()
    for copy in copies:
        copy.wait()


def on_device(ngy, ngx, tracer, east_speed, north_speed, columns, thickness, surface_flux, helm):
    f32 = jnp.float32
    any_spec = pl.BlockSpec(memory_space=pltpu.HBM)
    vmem = pl.BlockSpec(memory_space=pltpu.VMEM)
    results = pl.pallas_call(
        functools.partial(kernel, ngy, ngx),
        out_shape=(pltpu.VMEM((K, R, C), f32), pltpu.VMEM((R, C), f32)),
        in_specs=[any_spec, any_spec, any_spec, any_spec, any_spec, any_spec, any_spec],
        out_specs=(vmem, vmem),
        scratch_shapes=[
            pltpu.SMEM((K,), f32),
            pltpu.VMEM((NF, 2, RE, L), f32),
            pltpu.VMEM((2, RE, L), jnp.int32),
            pltpu.VMEM((2, RE, L), f32),
            pltpu.VMEM((9, RE, L), f32),
            pltpu.VMEM((K, 2, RE, L), f32),
            pltpu.VMEM((K, 2, RE, L), f32),
            pltpu.VMEM((2, RE, L), f32),
            pltpu.VMEM((2, RE, L), f32),
            pltpu.VMEM((2, RE, L), f32),
            pltpu.VMEM((2, RE, L), f32),
            pltpu.VMEM((2, RE, L), f32),
            pltpu.VMEM((2, RE, L), f32),
            pltpu.VMEM((RE, L), f32),
            pltpu.VMEM((RE, L), f32),
            pltpu.VMEM((3, RE, L), f32),
            pltpu.VMEM((RE, L), f32),
            pltpu.VMEM((R, L), f32),
            pltpu.VMEM((R, L), f32),
            pltpu.VMEM((RE, L), f32),
            pltpu.VMEM((RE, L), f32),
            pltpu.VMEM((3, RE, L), f32),
            pltpu.VMEM((3, RE, L), f32),
            pltpu.VMEM((3, RE, L), f32),
            pltpu.VMEM((3, 3, RE, L), f32),
            pltpu.VMEM((3, RE, L), f32),
            pltpu.VMEM((3, RE, L), f32),
            pltpu.VMEM((2, 1, L), f32),
            pltpu.VMEM((32, 1, L), f32),
            pltpu.VMEM((8, 1, L), f32),
            pltpu.SemaphoreType.DMA((K // PAIR + 2,)),
            pltpu.SemaphoreType.DMA((3,)),
            pltpu.SemaphoreType.DMA((3,)),
            pltpu.SemaphoreType.DMA((2,)),
            pltpu.SemaphoreType.DMA((2,)),
        ],
        compiler_params=pltpu.CompilerParams(collective_id=0, has_side_effects=True),
    )(tracer, east_speed, north_speed, columns, thickness, surface_flux, helm)
    return pl.pallas_call(
        put_kernel,
        out_shape=(jax.ShapeDtypeStruct((K, R, C), f32), jax.ShapeDtypeStruct((R, C), f32)),
        in_specs=[vmem, vmem],
        out_specs=(any_spec, any_spec),
        scratch_shapes=[pltpu.SemaphoreType.DMA((2,))],
    )(*[pltpu.with_memory_space_constraint(r, pltpu.VMEM) for r in results])


def solution(mesh):
    sizes = mesh.shape
    cells, plane = P(None, "gy", "gx"), P("gy", "gx")
    return jax.shard_map(
        functools.partial(on_device, sizes["gy"], sizes["gx"]),
        mesh=mesh,
        in_specs=(cells, cells, cells, plane, P(), plane, plane),
        out_specs=(cells, plane),
        check_vma=False,
    )
```

```python
import functools

import jax
import jax.numpy as jnp
from jax import lax
from jax.experimental import pallas as pl
from jax.experimental.pallas import tpu as pltpu
from jax.sharding import PartitionSpec as P

ITERS = 3
K = 8
R, C, L = 128, 256, 128
RE = R + 24
HALO = 5
SHIFT = 0.75
MESH = pl.DeviceIdType.MESH
TR, EA, NO, SF, HE, CO = 0, K, 2 * K, 3 * K, 3 * K + 1, 3 * K + 2
NF = 3 * K + 2
PAIR = 2


SLOT = 32
QUADS = 4
STARTS = {TR: (0, 14), EA: (5, 19), NO: (9, 23)}
WIDTHS = {TR: (5, 5), EA: (4, 5), NO: (4, 4)}
PLANES = ((CO, 27, 4), (SF, 59, 3), (HE, 91, 3))
S_SF, S_HE, S_CO = 6, 7, 8


def lane_plan():
    plan = [(field, at, width, width) for field, at, width in PLANES]
    for k in range(K):
        for base in (TR, EA, NO):
            plan.append((base + k, SLOT * (k % QUADS) + STARTS[base][k // QUADS]) + WIDTHS[base])
    return plan


PLAN = lane_plan()


def window(lane, start, width):
    start %= L
    if start + width <= L:
        return (lane >= start) & (lane < start + width)
    return (lane >= start) | (lane < start + width - L)


def turn(a, shift):
    shift %= L
    return pltpu.roll(a, shift, 1) if shift else a


def ring_east(tiles, lane):
    turned = [turn(a, -1) for a in tiles]
    if len(tiles) == 1:
        return turned
    return [jnp.where(lane < L - 1, a, turned[(i + 1) % len(tiles)]) for i, a in enumerate(turned)]


def ring_west(tiles, lane):
    turned = [turn(a, 1) for a in tiles]
    if len(tiles) == 1:
        return turned
    return [jnp.where(lane > 0, a, turned[i - 1]) for i, a in enumerate(turned)]


def rows(at):
    return pl.ds(at, 8)


def kernel(
    ngy, ngx,
    tr_hbm, ea_hbm, no_hbm, co_hbm, th_hbm, sf_hbm, he_hbm,
    tr_out, h_out,
    th, a, ci, cf, s, c1, c2, c1s, c2s, fl, fls, me_s, mn_s, mes_s, mns_s, fx, fs,
    pw, pe, re, rw, v0_s, v1_s, v2_s, sh_s, inv_s, wet_s, row, b1, b2,
    load_sem, send_sem, recv_sem, rs_sem, rr_sem,
):
    f32 = jnp.float32
    gy, gx = lax.axis_index("gy"), lax.axis_index("gx")
    north, south = lax.rem(gy + 1, ngy), lax.rem(gy + ngy - 1, ngy)
    e_id, w_id = lax.rem(gx + 1, ngx), lax.rem(gx + ngx - 1, ngx)
    hi, z = lax.div(gx, 8), lax.rem(gx, 8)
    group1 = [
        (lax.rem(gy + dy, ngy), lax.rem(gx + 8 * dh, ngx))
        for dh in range(2) for dy in range(16) if dy or dh
    ]
    def far_first(entry):
        dy, dh = (entry[0] + 1) % 16, (entry[0] + 1) // 16
        return -2 * dh - min(dy % 8, 8 - dy % 8)

    far1 = [device for i, device in sorted(enumerate(group1), key=far_first) if i not in (0, 14)]
    group2 = [(gy, hi * 8 + lax.rem(z + dz, 8)) for dz in range(1, 8)]
    near = [(north, gx), (south, gx), (gy, e_id), (gy, w_id),
            (north, e_id), (north, w_id), (south, e_id), (south, w_id)]

    barrier = pltpu.get_barrier_semaphore()

    def greet(devices):
        for y, x in devices:
            pl.semaphore_signal(barrier, inc=1, device_id={"gy": y, "gx": x}, device_id_type=MESH)

    greet(near)
    own, both = pl.ds(8, R), pl.ds(0, 2)
    halves = [pl.ds(0, L), pl.ds(L, L)]
    for src, dst in ((sf_hbm, a.at[SF]), (he_hbm, a.at[HE]), (co_hbm, ci)):
        for i, half in enumerate(halves):
            pltpu.make_async_copy(src.at[:, half], dst.at[i, own], load_sem.at[K // PAIR]).start()
    greet(far1 + group2)
    for g in range(K // PAIR):
        for src, base in ((tr_hbm, TR), (ea_hbm, EA), (no_hbm, NO)):
            for i, half in enumerate(halves):
                pltpu.make_async_copy(
                    src.at[pl.ds(PAIR * g, PAIR), :, half], a.at[pl.ds(base + PAIR * g, PAIR), i, own], load_sem.at[g]
                ).start()
    th_load = pltpu.make_async_copy(th_hbm, th, load_sem.at[K // PAIR + 1])
    th_load.start()

    def wait_rows(ref, sem):
        pltpu.make_async_copy(ref, ref, sem).wait()

    lane = lax.broadcasted_iota(jnp.int32, (8, L), 1)
    tiles = range(R // 8)

    packs = [[jnp.zeros((8, L), f32) for _ in tiles] for _ in range(2)]
    for g in range(-1, K // PAIR):
        wait_rows(a.at[pl.ds(0, 3 if g < 0 else 3 * PAIR), both, own], load_sem.at[g if g >= 0 else K // PAIR])
        if g < 0:
            for side in range(2):
                for t in tiles:
                    depth = ci[side, rows(8 + 8 * t), :].astype(f32)
                    beyond = turn(depth, -1)
                    if side:
                        beyond = jnp.where(lane == L - 1, float(K), beyond)
                    sh_s[0, side, rows(8 * t), :] = jnp.minimum(depth, beyond)
        begin = 0 if g < 0 else 3 + 3 * PAIR * g
        for field, at, first, last in PLAN[begin : begin + (3 if g < 0 else 3 * PAIR)]:
            for side in range(2):
                width = last if side else first
                mask = window(lane, at - 8 - width if side else at, width)
                shift = at - 8 if side else at
                for t in tiles:
                    if field == CO:
                        value = ci[side, rows(8 + 8 * t), :].astype(f32)
                    else:
                        value = a[field, side, rows(8 + 8 * t), :]
                    if EA <= field < NO:
                        value = jnp.where(sh_s[0, side, rows(8 * t), :] > float(field - EA), value, 0.0)
                    packs[side][t] = jnp.where(mask, turn(value, shift), packs[side][t])
    for side, dest in enumerate((pw, pe)):
        for t in tiles:
            dest[rows(8 * t), :] = packs[side][t]

    pl.semaphore_wait(barrier, len(near) + len(far1) + len(group2))

    top, bottom = pl.ds(R + 3, HALO), pl.ds(8, HALO)
    ghost_s, ghost_n = pl.ds(3, HALO), pl.ds(R + 8, HALO)
    every = pl.ds(0, NF)

    def send(kind, src, dst, y, x):
        pltpu.make_async_remote_copy(
            src_ref=src, dst_ref=dst, send_sem=send_sem.at[kind], recv_sem=recv_sem.at[kind],
            device_id={"gy": y, "gx": x}, device_id_type=MESH,
        ).start()

    has_north, has_south = gy < ngy - 1, gy > 0

    @pl.when(has_north)
    def _():
        send(1, pe.at[pl.ds(R - HALO, HALO)], rw.at[ghost_s], north, e_id)
        send(1, pw.at[pl.ds(R - HALO, HALO)], re.at[ghost_s], north, w_id)

    @pl.when(has_south)
    def _():
        send(2, pe.at[pl.ds(0, HALO)], rw.at[ghost_n], south, e_id)
        send(2, pw.at[pl.ds(0, HALO)], re.at[ghost_n], south, w_id)

    send(0, pe, rw.at[own], gy, e_id)
    send(0, pw, re.at[own], gy, w_id)

    @pl.when(has_north)
    def _():
        send(1, ci.at[both, top], ci.at[both, ghost_s], north, gx)
        send(1, a.at[every, both, top], a.at[every, both, ghost_s], north, gx)

    @pl.when(has_south)
    def _():
        send(2, ci.at[both, bottom], ci.at[both, ghost_n], south, gx)
        send(2, a.at[every, both, bottom], a.at[every, both, ghost_n], south, gx)

    column_rows = (1, 2, R)
    row_rows = (1, 2, HALO * (NF + 2))
    assert RE >= HALO * (NF + 2)

    def sized(shape):
        return c1.at[pl.ds(0, shape[0]), pl.ds(0, shape[1]), pl.ds(0, shape[2])]

    def each_end(sem):
        @pl.when(has_north if sem is send_sem else has_south)
        def _():
            wait_rows(sized(row_rows), sem.at[1])

        @pl.when(has_south if sem is send_sem else has_north)
        def _():
            wait_rows(sized(row_rows), sem.at[2])

    zero8 = jnp.zeros((8, L), f32)
    for at0, open_end in ((0, has_south), (R + 8, has_north)):

        @pl.when(jnp.logical_not(open_end))
        def _(at0=at0):
            for i in range(2):
                ci[i, rows(at0), :] = jnp.zeros((8, L), jnp.int32)
                for field in range(NF):
                    a[field, i, rows(at0), :] = zero8
            re[rows(at0), :] = zero8
            rw[rows(at0), :] = zero8

    th_load.wait()

    def seam(field, at):
        left, right = (cf[0, rows(at), :], cf[1, rows(at), :]) if field == CO else (
            a[field, 0, rows(at), :], a[field, 1, rows(at), :])
        return jnp.where(lane < 64, turn(right, 4), turn(left, -4))

    def seam_quad(base, half, at):
        tile = jnp.zeros((8, L), f32)
        for q in range(QUADS):
            field = base + QUADS * half + q
            tile = jnp.where(window(lane, SLOT * q, 4), turn(a[field, 1, rows(at), :], SLOT * q + 4), tile)
            tile = jnp.where(window(lane, SLOT * q - 4, 4), turn(a[field, 0, rows(at), :], SLOT * q - 4), tile)
        return tile

    quads = [(base, half) for base in (TR, EA, NO) for half in range(2)]
    planes = ((S_SF, SF), (S_HE, HE), (S_CO, CO))

    def own_seam(tile, at):
        return seam_quad(*quads[tile], at) if tile < 6 else seam(planes[tile - 6][1], at)

    def diagonal(i, at, helm, depth):
        inv_s[i, rows(at), :] = 1.0 / (6.0 + helm)
        wet_s[i, rows(at), :] = jnp.where(depth > 0.0, 1.0, 0.0)

    for i in range(2):
        for t in tiles:
            at = 8 + 8 * t
            cf[i, rows(at), :] = ci[i, rows(at), :].astype(f32)
            fx[i, rows(at), :] = a[SF, i, rows(at), :]
            diagonal(i, at, a[HE, i, rows(at), :], cf[i, rows(at), :])
    for tile in range(9):
        for t in tiles:
            s[tile, rows(8 + 8 * t), :] = own_seam(tile, 8 + 8 * t)

    def face_masks(at, below):
        depth = [cf[i, rows(at), :] for i in range(2)]
        for i, other in enumerate(ring_east(depth, lane)):
            me_s[i, rows(at), :] = jnp.minimum(depth[i], other)
            mn_s[i, rows(below), :] = jnp.minimum(cf[i, rows(below), :], cf[i, rows(below + 1), :])

    for t in tiles:
        face_masks(8 + 8 * t, min(8 + 8 * t, R - 1))

    def north_flux(k, kf, i, current, at):
        speed = jnp.where(mn_s[i, rows(at), :] > kf, a[NO + k, i, rows(at), :], 0.0)
        return speed * jnp.where(speed > 0.0, current(i, at), current(i, at + 1))

    def east_flux(k, kf, now, at):
        out = []
        for i, other in enumerate(ring_east(now, lane)):
            speed = jnp.where(me_s[i, rows(at), :] > kf, a[EA + k, i, rows(at), :], 0.0)
            out.append(speed * jnp.where(speed > 0.0, now[i], other))
        return out

    def own_step(k, kf, current, store, starts, direct):
        if not direct:
            for at in [at - 1 for at in starts] + [starts[-1]]:
                for i in range(2):
                    fl[i, rows(at), :] = north_flux(k, kf, i, current, at)
        for at in starts:
            now = [current(i, at) for i in range(2)]
            fe = east_flux(k, kf, now, at)
            fw = ring_west(fe, lane)
            for i in range(2):
                if direct:
                    fn, fb = north_flux(k, kf, i, current, at), north_flux(k, kf, i, current, at - 1)
                else:
                    fn, fb = fl[i, rows(at), :], fl[i, rows(at - 1), :]
                store(i, at, now[i] - (fe[i] - fw[i] + fn - fb))

    def own_levels(k, starts1, starts2, direct):
        kf = float(k) if isinstance(k, int) else k.astype(f32)
        weight = th[k]

        def put1(i, at, value):
            c1[k, i, rows(at), :] = value

        def put2(i, at, value):
            c2[k, i, rows(at), :] = value
            fx[i, rows(at), :] += jnp.where(cf[i, rows(at), :] > kf, weight * value, 0.0)

        own_step(k, kf, lambda i, at: a[TR + k, i, rows(at), :], put1, starts1, direct)
        own_step(k, kf, lambda i, at: c1[k, i, rows(at), :], put2, starts2, direct)

    starts1 = [9 + 8 * t for t in range(15)] + [R - 1]
    starts2 = [12 + 8 * t for t in range(15)]

    def interior(k, carry):
        own_levels(k, starts1, starts2, False)
        return carry

    lax.fori_loop(0, K, interior, 0)

    wait_rows(sized(column_rows), recv_sem.at[0])

    within = lane & (SLOT - 1)
    ghosts = ((within >= 4) & (within < 9)) | ((within >= 23) & (within < 28))
    near_ghosts = window(lane, 4, 4) | window(lane, 120, 4)
    outer_ghosts = window(lane, 8, 1) | window(lane, 119, 1)
    own_lanes = window(lane, 124, 8)
    ends = (0, R + 8)

    def unpack(spots, beneath):
        from_east = [re[rows(at), :] for at in spots]
        from_west = [rw[rows(at), :] for at in spots]
        for tile in range(9):
            if tile < 6:
                base, half = quads[tile]
                start = STARTS[base][half]
                mask = ((lane - start) & (SLOT - 1)) < WIDTHS[base][0]
            else:
                start, width = {SF: (59, 3), HE: (91, 3), CO: (27, 4)}[planes[tile - 6][1]]
                mask = window(lane, start, width)
            for j, spot in enumerate(spots):
                value = turn(jnp.where(mask, from_east[j], from_west[j]), 4 - start)
                below = beneath(tile, spot)
                if tile == S_CO:
                    value = jnp.where(near_ghosts, value, jnp.where(own_lanes, below, 0.0))
                    value = jnp.where(outer_ghosts, float(K), value)
                    value = value + turn(value, SLOT) + turn(value, 2 * SLOT) + turn(value, 3 * SLOT)
                else:
                    value = jnp.where(ghosts, value, below)
                s[tile, rows(spot), :] = value

    for first_row in (8, 72):
        unpack([first_row + 8 * t for t in range(8)], lambda tile, at: s[tile, rows(at), :])

    def beside(tile):
        return turn(tile, 4), turn(tile, -4)

    def ghost_tile(field, at):
        west, east = beside(s[field, rows(at), :])
        return jnp.where(lane < 64, east, west)

    for t in tiles:
        at = 8 + 8 * t
        depth = s[S_CO, rows(at), :]
        mes_s[rows(at), :] = jnp.minimum(depth, turn(depth, -1))
        below = min(at, R - 1)
        mns_s[rows(below), :] = jnp.minimum(s[S_CO, rows(below), :], s[S_CO, rows(below + 1), :])
        fs[rows(at), :] = zero8
        diagonal(2, at, ghost_tile(S_HE, at), ghost_tile(S_CO, at))

    slot = ((lane + SLOT // 2) // SLOT) & (QUADS - 1)
    floors = [(slot + QUADS * half).astype(f32) for half in range(2)]
    weights = []
    for half in range(2):
        weight = jnp.zeros((8, L), f32)
        for q in range(QUADS):
            weight = jnp.where(slot == q, th[QUADS * half + q], weight)
        weights.append(weight)

    def seam_flux(half, current, at):
        speed = jnp.where(mns_s[rows(at), :] > floors[half], s[4 + half, rows(at), :], 0.0)
        return speed * jnp.where(speed > 0.0, current(at), current(at + 1))

    def seam_step(half, current, store, starts, direct):
        if not direct:
            for at in [at - 1 for at in starts] + [starts[-1]]:
                fls[half, rows(at), :] = seam_flux(half, current, at)
        for at in starts:
            now = current(at)
            speed = jnp.where(mes_s[rows(at), :] > floors[half], s[2 + half, rows(at), :], 0.0)
            fe = speed * jnp.where(speed > 0.0, now, turn(now, -1))
            if direct:
                fn, fb = seam_flux(half, current, at), seam_flux(half, current, at - 1)
            else:
                fn, fb = fls[half, rows(at), :], fls[half, rows(at - 1), :]
            store(at, now - (fe - turn(fe, 1) + fn - fb))

    def seam_levels(half, starts1, starts2, direct):
        def put1(at, value):
            c1s[half, rows(at), :] = value

        def put2(at, value):
            c2s[half, rows(at), :] = value
            fs[rows(at), :] += jnp.where(s[S_CO, rows(at), :] > floors[half], weights[half] * value, 0.0)

        seam_step(half, lambda at: s[half, rows(at), :], put1, starts1, direct)
        seam_step(half, lambda at: c1s[half, rows(at), :], put2, starts2, direct)

    for half in range(2):
        seam_levels(half, starts1, starts2, False)

    each_end(recv_sem)

    for at in ends:
        for i in range(2):
            cf[i, rows(at), :] = ci[i, rows(at), :].astype(f32)
    unpack(ends, own_seam)

    strips = (4, R + 4)
    for at in strips:
        face_masks(at, at - 1)
        below = at + 1
        for i in range(2):
            mn_s[i, rows(below), :] = jnp.minimum(cf[i, rows(below), :], cf[i, rows(below + 1), :])
            fx[i, rows(at), :] = a[SF, i, rows(at), :]
        depth = s[S_CO, rows(at), :]
        mes_s[rows(at), :] = jnp.minimum(depth, turn(depth, -1))
        for below in (at - 1, at + 1):
            mns_s[rows(below), :] = jnp.minimum(s[S_CO, rows(below), :], s[S_CO, rows(below + 1), :])
        fs[rows(at), :] = zero8
    for at in ends:
        for i in range(2):
            diagonal(i, at, a[HE, i, rows(at), :], cf[i, rows(at), :])
        diagonal(2, at, ghost_tile(S_HE, at), ghost_tile(S_CO, at))

    for half in range(2):
        seam_levels(half, strips, strips, True)
    for k in range(K):
        own_levels(k, strips, strips, True)

    blocks = [1] + [8 * t for t in range(1, 18)]
    inside = [8 * t for t in range(1, 17)]

    for at in blocks:
        folded = fs[rows(at), :]
        folded = folded + turn(folded, SLOT) + turn(folded, 2 * SLOT) + turn(folded, 3 * SLOT)
        f_w, f_e = beside(folded + s[S_SF, rows(at), :])
        forcing = [
            jnp.where(lane < 2, f_w, fx[0, rows(at), :]),
            jnp.where(lane >= L - 2, f_e, fx[1, rows(at), :]),
            jnp.where(lane < 64, f_e, f_w),
        ]
        for i in range(3):
            fx[i, rows(at), :] = forcing[i]
            v0_s[i, rows(at), :] = forcing[i] * inv_s[i, rows(at), :]

    nu = [[jnp.zeros((8, L), f32) for _ in range(2)] for _ in range(6)]

    def operator(n, src, spots, store):
        spread = {}
        for at in blocks:
            w = [wet_s[i, rows(at), :] * src[i, rows(at), :] for i in range(3)]
            h = [x + y for x, y in zip(ring_west(w, lane), ring_east(w, lane))]
            spread[at] = h
            for i in range(3):
                sh_s[n, i, rows(at), :] = w[i] + 0.5 * h[i]
        for at in spots:
            for i in range(3):
                u = wet_s[i, rows(at), :] * (
                    spread[at][i] + sh_s[n, i, rows(at + 1), :] + sh_s[n, i, rows(at - 1), :])
                store(i, at, u)

    def counted(i, at):
        return i < 2 and at in inside

    def store1(i, at, u):
        f = fx[i, rows(at), :]
        g = u - SHIFT * f
        v = g * inv_s[i, rows(at), :]
        v1_s[i, rows(at), :] = v
        sh_s[2, i, rows(at), :] = g
        if counted(i, at):
            nu[0][i] += f * v0_s[i, rows(at), :]
            nu[1][i] += v * f
            nu[2][i] += v * g

    def store2(i, at, u):
        g = u - SHIFT * sh_s[2, i, rows(at), :]
        v = g * inv_s[i, rows(at), :]
        v2_s[i, rows(at), :] = v
        sh_s[0, i, rows(at), :] = g
        if counted(i, at):
            nu[3][i] += v1_s[i, rows(at), :] * g
            nu[4][i] += v * g

    def store3(i, at, u):
        if counted(i, at):
            nu[5][i] += v2_s[i, rows(at), :] * (u - SHIFT * sh_s[0, i, rows(at), :])

    operator(0, v0_s, blocks, store1)
    operator(1, v1_s, blocks, store2)
    operator(2, v2_s, inside, store3)

    def finish_tracer():
        def put(half, carry):
            for q in range(QUADS):
                k = QUADS * half + q
                for t in tiles:
                    at = 8 + 8 * t
                    patch = c2s[half, rows(at), :]
                    patches = turn(patch, 4 - SLOT * q), turn(patch, -4 - SLOT * q)
                    for i, mask in enumerate((lane < 2, lane >= L - 2)):
                        tr_out[k, rows(8 * t), halves[i]] = jnp.where(mask, patches[i], c2[k, i, rows(at), :])
            return carry

        lax.fori_loop(0, K // QUADS, put, 0)

    lane1 = lax.broadcasted_iota(jnp.int32, (1, 128), 1)
    packed = jnp.zeros((1, 128), jnp.float32)
    for i, part in enumerate(nu):
        lanes = jnp.sum(part[0] + part[1], axis=0, keepdims=True)
        total = jnp.sum(lanes, axis=1, keepdims=True)
        packed = jnp.where(lane1 == i, total, packed)

    reduce_sends = []
    for i, (group, slot, buf) in enumerate(((group1, gy * 2 + hi, b1), (group2, z, b2))):
        row[i] = packed
        n = len(group)
        for y, x in group:
            copy = pltpu.make_async_remote_copy(
                src_ref=row.at[i], dst_ref=buf.at[slot], send_sem=rs_sem.at[i], recv_sem=rr_sem.at[i],
                device_id={"gy": y, "gx": x}, device_id_type=MESH,
            )
            copy.start()
        buf[slot] = packed
        if i == 0:
            finish_tracer()
        pltpu.make_async_copy(buf.at[pl.ds(0, n)], buf.at[pl.ds(0, n)], rr_sem.at[i]).wait()
        reduce_sends.append((buf, n, i))
        packed = jnp.sum(buf[...], axis=0)

    m = [jnp.sum(jnp.where(lane1 == i, packed, 0.0), axis=1, keepdims=True) for i in range(6)]

    def form(p, moments):
        total = None
        for i, pi in enumerate(p):
            for j, pj in enumerate(p[i:], i):
                term = (pi * pj if i == j else 2.0 * pi * pj) * moments[i + j]
                total = term if total is None else total + term
        return total

    diff = [(1.0 - SHIFT) * m[i] - m[i + 1] for i in range(5)]
    one = jnp.ones_like(m[0])
    zc, pc = [one], [one]
    heights = [jnp.zeros_like(one)] * 3
    rz = m[0]
    for it in range(ITERS):
        alpha = rz / form(pc, diff)
        heights = [h + alpha * pc[i] if i < len(pc) else h for i, h in enumerate(heights)]
        if it + 1 < ITERS:
            applied = [(1.0 - SHIFT) * p - q for p, q in zip(pc + [jnp.zeros_like(one)], [jnp.zeros_like(one)] + pc)]
            zc = [(zc[i] if i < len(zc) else 0.0) - alpha * applied[i] for i in range(len(applied))]
            rz_next = form(zc, m)
            beta = rz_next / rz
            pc = [zc[i] + beta * pc[i] if i < len(pc) else zc[i] for i in range(len(zc))]
            rz = rz_next

    for t in tiles:
        at = 8 + 8 * t
        for i in range(2):
            h_out[rows(8 * t), halves[i]] = (
                heights[0] * v0_s[i, rows(at), :] + heights[1] * v1_s[i, rows(at), :] + heights[2] * v2_s[i, rows(at), :])

    wait_rows(sized(column_rows), send_sem.at[0])
    each_end(send_sem)
    for buf, n, i in reduce_sends:
        pltpu.make_async_copy(buf.at[pl.ds(0, n)], buf.at[pl.ds(0, n)], rs_sem.at[i]).wait()


def put_kernel(tr, h, tr_hbm, h_hbm, sem):
    copies = [pltpu.make_async_copy(tr, tr_hbm, sem.at[0]), pltpu.make_async_copy(h, h_hbm, sem.at[1])]
    for copy in copies:
        copy.start()
    for copy in copies:
        copy.wait()


def on_device(ngy, ngx, tracer, east_speed, north_speed, columns, thickness, surface_flux, helm):
    f32 = jnp.float32
    any_spec = pl.BlockSpec(memory_space=pltpu.HBM)
    vmem = pl.BlockSpec(memory_space=pltpu.VMEM)
    results = pl.pallas_call(
        functools.partial(kernel, ngy, ngx),
        out_shape=(pltpu.VMEM((K, R, C), f32), pltpu.VMEM((R, C), f32)),
        in_specs=[any_spec, any_spec, any_spec, any_spec, any_spec, any_spec, any_spec],
        out_specs=(vmem, vmem),
        scratch_shapes=[
            pltpu.SMEM((K,), f32),
            pltpu.VMEM((NF, 2, RE, L), f32),
            pltpu.VMEM((2, RE, L), jnp.int32),
            pltpu.VMEM((2, RE, L), f32),
            pltpu.VMEM((9, RE, L), f32),
            pltpu.VMEM((K, 2, RE, L), f32),
            pltpu.VMEM((K, 2, RE, L), f32),
            pltpu.VMEM((2, RE, L), f32),
            pltpu.VMEM((2, RE, L), f32),
            pltpu.VMEM((2, RE, L), f32),
            pltpu.VMEM((2, RE, L), f32),
            pltpu.VMEM((2, RE, L), f32),
            pltpu.VMEM((2, RE, L), f32),
            pltpu.VMEM((RE, L), f32),
            pltpu.VMEM((RE, L), f32),
            pltpu.VMEM((3, RE, L), f32),
            pltpu.VMEM((RE, L), f32),
            pltpu.VMEM((R, L), f32),
            pltpu.VMEM((R, L), f32),
            pltpu.VMEM((RE, L), f32),
            pltpu.VMEM((RE, L), f32),
            pltpu.VMEM((3, RE, L), f32),
            pltpu.VMEM((3, RE, L), f32),
            pltpu.VMEM((3, RE, L), f32),
            pltpu.VMEM((3, 3, RE, L), f32),
            pltpu.VMEM((3, RE, L), f32),
            pltpu.VMEM((3, RE, L), f32),
            pltpu.VMEM((2, 1, L), f32),
            pltpu.VMEM((32, 1, L), f32),
            pltpu.VMEM((8, 1, L), f32),
            pltpu.SemaphoreType.DMA((K // PAIR + 2,)),
            pltpu.SemaphoreType.DMA((3,)),
            pltpu.SemaphoreType.DMA((3,)),
            pltpu.SemaphoreType.DMA((2,)),
            pltpu.SemaphoreType.DMA((2,)),
        ],
        compiler_params=pltpu.CompilerParams(collective_id=0, has_side_effects=True),
    )(tracer, east_speed, north_speed, columns, thickness, surface_flux, helm)
    return pl.pallas_call(
        put_kernel,
        out_shape=(jax.ShapeDtypeStruct((K, R, C), f32), jax.ShapeDtypeStruct((R, C), f32)),
        in_specs=[vmem, vmem],
        out_specs=(any_spec, any_spec),
        scratch_shapes=[pltpu.SemaphoreType.DMA((2,))],
    )(*[pltpu.with_memory_space_constraint(r, pltpu.VMEM) for r in results])


def solution(mesh):
    sizes = mesh.shape
    cells, plane = P(None, "gy", "gx"), P("gy", "gx")
    return jax.shard_map(
        functools.partial(on_device, sizes["gy"], sizes["gx"]),
        mesh=mesh,
        in_specs=(cells, cells, cells, plane, P(), plane, plane),
        out_specs=(cells, plane),
        check_vma=False,
    )
```
